128 devices in a mesh: data: 1, expert: 128 (over z, y, x, core).
Axes of the slice: x: 4, y: 4, z: 4, core: 2. Of those that a mesh axis runs over, the one named last changes fastest.
Arguments:
- tokens: bfloat16 [16384, 2048], P(('data', 'expert'))
- expert_ids: int32 [16384, 8], P(('data', 'expert'))
- gate_wts: float32 [16384, 8], P(('data', 'expert'))
- dev_slot: int32 [16384, 8], P(('data', 'expert'))
- exp_slot: int32 [16384, 8], P(('data', 'expert'))
- w_gate: bfloat16 [128, 2048, 768], P('expert')
- w_up: bfloat16 [128, 2048, 768], P('expert')
- w_down: bfloat16 [128, 768, 2048], P('expert')
Outputs:
- output: bfloat16 [16384, 2048], P(('data', 'expert'))
All inputs are finite; a program needn't handle non-finite values.
Results may differ from the reference program's by a relative error of at most 0.00784482.
Values are sent between devices in bfloat16 or wider.
A program may use at most 1 GiB of HBM per device.

```python
import jax
import jax.numpy as jnp
from jax import lax

TOK_DEV = 128
GROUP_SIZE = 128
D_MODEL = 2048
D_FF = 768
N_EXPERTS = 128
TOP_K = 8

TOKENS = TOK_DEV * GROUP_SIZE
E_LOCAL = N_EXPERTS // GROUP_SIZE
DEV_CAP = min(TOK_DEV, 8 * ((3 * TOK_DEV * TOP_K + 16 * GROUP_SIZE - 1) // (16 * GROUP_SIZE)))
EXP_CAP = 8 * ((TOKENS * TOP_K + 4 * N_EXPERTS - 1) // (4 * N_EXPERTS))
HOT_ROWS = (EXP_CAP + GROUP_SIZE - 1) // GROUP_SIZE
N_ROWS = GROUP_SIZE * DEV_CAP


def draw_routing(key):
    noise_key, skew_key = jax.random.split(key)
    noise_int = jax.random.randint(noise_key, (TOKENS, N_EXPERTS), 0, 1024)
    skew_bias = jax.random.randint(skew_key, (N_EXPERTS,), 0, 512)
    tok_pos = jnp.arange(TOKENS) % TOK_DEV
    src_dev = jnp.arange(TOKENS) // TOK_DEV
    ex_range = jnp.arange(N_EXPERTS)
    fwd_expert = ((src_dev + 1) % GROUP_SIZE) * E_LOCAL + tok_pos % E_LOCAL
    forced = (ex_range[None, :] == fwd_expert[:, None]) & (tok_pos[:, None] < DEV_CAP)
    hot_pick = (ex_range[None, :] == 0) & (tok_pos[:, None] < HOT_ROWS)
    score_int = noise_int + skew_bias[None, :] + 4096 * (forced | hot_pick).astype(jnp.int32)
    ranked = score_int * N_EXPERTS + ex_range[None, :]
    expert_ids = lax.top_k(ranked, TOP_K)[1].astype(jnp.int32)
    owner_dev = expert_ids // E_LOCAL
    dev_range = jnp.arange(GROUP_SIZE)

    def source_rank(src_owner):
        touch_dev = jnp.any(src_owner[:, :, None] == dev_range[None, None, :], axis=1).astype(jnp.int32)
        before = jnp.cumsum(touch_dev, axis=0) - touch_dev
        return jnp.take_along_axis(before, src_owner, axis=1)

    dev_rank = lax.map(source_rank, owner_dev.reshape(GROUP_SIZE, TOK_DEV, TOP_K)).reshape(TOKENS, TOP_K)
    dev_keep = dev_rank < DEV_CAP
    exp_loads = jnp.zeros((TOKENS, N_EXPERTS), jnp.int32).at[jnp.arange(TOKENS)[:, None], expert_ids].add(dev_keep.astype(jnp.int32))
    exp_before = jnp.cumsum(exp_loads, axis=0) - exp_loads
    exp_rank = jnp.take_along_axis(exp_before, expert_ids, axis=1)
    kept_choice = dev_keep & (exp_rank < EXP_CAP)
    dev_slot = jnp.where(kept_choice, dev_rank, -1).astype(jnp.int32)
    exp_slot = jnp.where(kept_choice, exp_rank, -1).astype(jnp.int32)
    return expert_ids, dev_slot, exp_slot


def setup_inputs(seed: int = 0, part: int = 0) -> dict:
    base_key = jax.random.key(seed)
    part_key = jax.random.fold_in(base_key, part)
    tok_key, gate_key, route_key = jax.random.split(part_key, 3)
    wg_key, wu_key, wd_key = jax.random.split(jax.random.fold_in(base_key, 1000), 3)
    tokens = jax.random.normal(tok_key, (TOKENS, D_MODEL), jnp.float32).astype(jnp.bfloat16)
    gate_wts = (0.5 + jax.random.uniform(gate_key, (TOKENS, TOP_K), jnp.float32)) * TOP_K ** -0.5
    expert_ids, dev_slot, exp_slot = draw_routing(route_key)
    w_gate = (jax.random.normal(wg_key, (N_EXPERTS, D_MODEL, D_FF), jnp.float32) * D_MODEL ** -0.5).astype(jnp.bfloat16)
    w_up = (jax.random.normal(wu_key, (N_EXPERTS, D_MODEL, D_FF), jnp.float32) * D_MODEL ** -0.5).astype(jnp.bfloat16)
    w_down = (jax.random.normal(wd_key, (N_EXPERTS, D_FF, D_MODEL), jnp.float32) * D_FF ** -0.5).astype(jnp.bfloat16)
    return {"tokens": tokens, "expert_ids": expert_ids, "gate_wts": gate_wts, "dev_slot": dev_slot, "exp_slot": exp_slot, "w_gate": w_gate, "w_up": w_up, "w_down": w_down}


def reference(tokens, expert_ids, gate_wts, dev_slot, exp_slot, w_gate, w_up, w_down):
    owner_dev = expert_ids // E_LOCAL
    local_ex = expert_ids % E_LOCAL
    src_dev = (jnp.arange(TOKENS) // TOK_DEV)[:, None]
    row_idx = src_dev * DEV_CAP + dev_slot
    gate_bf = gate_wts.astype(jnp.bfloat16).astype(jnp.float32)
    tok_f32 = tokens.astype(jnp.float32)
    gate_all = w_gate.reshape(GROUP_SIZE, E_LOCAL, D_MODEL, D_FF)
    up_all = w_up.reshape(GROUP_SIZE, E_LOCAL, D_MODEL, D_FF)
    down_all = w_down.reshape(GROUP_SIZE, E_LOCAL, D_FF, D_MODEL)

    def device_step(out_acc, dest_dev):
        on_dest = (owner_dev == dest_dev) & (dev_slot >= 0)
        tok_row = jnp.max(jnp.where(on_dest, row_idx, -1), axis=1)
        tok_dest = jnp.where(tok_row >= 0, tok_row, N_ROWS)
        recv_rows = jnp.zeros((N_ROWS, D_MODEL), jnp.float32).at[tok_dest].add(tok_f32, mode="drop")
        recv_rows = recv_rows.astype(jnp.bfloat16).astype(jnp.float32)
        choice_ok = on_dest & (exp_slot >= 0)
        flat_ex = jnp.where(choice_ok, local_ex, E_LOCAL).reshape(-1)
        flat_pos = jnp.where(choice_ok, exp_slot, 0).reshape(-1)
        row_of = jnp.full((E_LOCAL, EXP_CAP), -1, jnp.int32).at[flat_ex, flat_pos].max(row_idx.reshape(-1), mode="drop")
        gate_of = jnp.zeros((E_LOCAL, EXP_CAP), jnp.float32).at[flat_ex, flat_pos].add(gate_bf.reshape(-1), mode="drop")
        filled = row_of >= 0
        exp_in = jnp.where(filled[:, :, None], recv_rows[jnp.maximum(row_of, 0)], 0.0)
        w_one = gate_all[dest_dev].astype(jnp.float32)
        w_two = up_all[dest_dev].astype(jnp.float32)
        w_three = down_all[dest_dev].astype(jnp.float32)
        hid_gate = jnp.einsum("esd,edf->esf", exp_in, w_one)
        hid_up = jnp.einsum("esd,edf->esf", exp_in, w_two)
        hidden = (jax.nn.silu(hid_gate) * hid_up).astype(jnp.bfloat16).astype(jnp.float32)
        exp_out = jnp.einsum("esf,efd->esd", hidden, w_three).astype(jnp.bfloat16).astype(jnp.float32)
        back_dest = jnp.where(filled, row_of, N_ROWS).reshape(-1)
        weighted = (gate_of[:, :, None] * exp_out).reshape(-1, D_MODEL)
        z_rows = jnp.zeros((N_ROWS, D_MODEL), jnp.float32).at[back_dest].add(weighted, mode="drop")
        z_rows = z_rows.astype(jnp.bfloat16).astype(jnp.float32)
        back_rows = jnp.where((tok_row >= 0)[:, None], z_rows[jnp.maximum(tok_row, 0)], 0.0)
        return out_acc + back_rows, None

    out_acc, unused_stack = lax.scan(device_step, jnp.zeros((TOKENS, D_MODEL), jnp.float32), jnp.arange(GROUP_SIZE))
    return out_acc.astype(jnp.bfloat16)
```

```python
import jax
import jax.numpy as jnp
from jax import lax
from jax.sharding import PartitionSpec as P


def solution(mesh):
    groups = mesh.shape["expert"]
    row_spec = P(("data", "expert"), None)
    weight_spec = P("expert", None, None)

    def device_layer(tokens, expert_ids, gate_wts, dev_slot, exp_slot, w_gate, w_up, w_down):
        tok_dev, top_k = expert_ids.shape
        d_model = tokens.shape[1]
        cap = min(tok_dev, 8 * ((3 * tok_dev * top_k + 16 * groups - 1) // (16 * groups)))
        n_rows = groups * cap
        kept = (dev_slot >= 0) & (exp_slot >= 0)
        dest = jnp.where(kept, expert_ids * cap + dev_slot, -1)
        hit = jnp.arange(n_rows)[:, None, None] == dest[None, :, :]
        pick = jnp.any(hit, axis=2).astype(jnp.bfloat16)
        gate_bf = gate_wts.astype(jnp.bfloat16).astype(jnp.float32)
        row_gate = jnp.sum(jnp.where(hit, gate_bf[None], 0.0), axis=(1, 2))
        send = jnp.dot(pick, tokens, preferred_element_type=jnp.float32).astype(jnp.bfloat16)
        recv = lax.all_to_all(send.reshape(groups, cap, d_model), "expert", 0, 0, tiled=True)
        x = recv.reshape(n_rows, d_model)
        hid_gate = jnp.dot(x, w_gate[0], preferred_element_type=jnp.float32)
        hid_up = jnp.dot(x, w_up[0], preferred_element_type=jnp.float32)
        hidden = (jax.nn.silu(hid_gate) * hid_up).astype(jnp.bfloat16)
        y = jnp.dot(hidden, w_down[0], preferred_element_type=jnp.float32).astype(jnp.bfloat16)
        back = lax.all_to_all(y.reshape(groups, cap, d_model), "expert", 0, 0, tiled=True)
        z = (back.reshape(n_rows, d_model).astype(jnp.float32) * row_gate[:, None]).astype(jnp.bfloat16)
        out = jnp.einsum("rt,rd->td", pick, z, preferred_element_type=jnp.float32)
        return out.astype(jnp.bfloat16)

    def moe_layer(*args):
        return jax.shard_map(device_layer, mesh=mesh, in_specs=(row_spec,) * 5 + (weight_spec,) * 3, out_specs=row_spec, check_vma=False)(*args)

    return moe_layer
```

```python
import jax
import jax.numpy as jnp
from jax import lax
from jax.experimental import pallas as pl
from jax.experimental.pallas import tpu as pltpu
from jax.sharding import PartitionSpec as P

STRIDE = (32, 8, 2)
RING = 4
SLOTS = 16
VMEM_CAP = 67043328
BF16 = jnp.bfloat16
F32 = jnp.float32


def rem4(v):
    return lax.rem(v, RING)


class Place:
    def __init__(self):
        self.me = lax.axis_index("expert")
        self.core = lax.rem(self.me, 2)
        self.k = [rem4(lax.div(self.me, s)) for s in STRIDE]

    def peer(self, axis, delta, core=None):
        there = rem4(self.k[axis] + delta + RING)
        dev = self.me + (there - self.k[axis]) * STRIDE[axis]
        return dev if core is None else dev + core - self.core

    def partner(self):
        return self.me + 1 - 2 * self.core

    def barrier(self):
        sem = pltpu.get_barrier_semaphore()
        peers = [self.peer(ax, dl, c) for ax in range(3) for dl in (1, -1) for c in (0, 1)] + [self.partner()]
        for dev in peers:
            pl.semaphore_signal(sem, inc=1, device_id={"expert": dev}, device_id_type=pl.DeviceIdType.MESH)
        pl.semaphore_wait(sem, len(peers))


def remote(src, dst, send, recv, dev):
    return pltpu.make_async_remote_copy(
        src_ref=src, dst_ref=dst, send_sem=send, recv_sem=recv, device_id={"expert": dev}, device_id_type=pl.DeviceIdType.MESH
    )


class Exchange:
    def __init__(self, pc, c, src, land, transit, send, recv, base):
        self.pc, self.c, self.src, self.land, self.transit = pc, c, src, land, transit
        self.send, self.recv, self.base = send, recv, base

    def sems(self, j, s, r):
        at = self.base + j * 9
        return self.send.at[at + s], self.recv.at[at + r]

    def first(self, j):
        pc, c = self.pc, self.c
        kc, h = pc.k[c], pc.core
        mine = self.land.at[j * 8 + kc * 2 + h]
        out = []
        far = rem4(kc + 2)
        for d, dl in enumerate((1, -1)):
            s, r = self.sems(j, 5 + d, 5 + d)
            out.append(remote(self.src.at[j * 8 + far * 2 + d], self.transit.at[d, j], s, r, pc.peer(c, dl)))
        for d, dl in enumerate((1, -1)):
            near = rem4(kc + dl + RING)
            for core in range(2):
                s, r = self.sems(j, 1 + d * 2 + core, 1 + d * 2 + h)
                out.append(remote(self.src.at[j * 8 + near * 2 + core], mine, s, r, pc.peer(c, dl, core)))
        s, r = self.sems(j, 0, 0)
        out.append(remote(self.src.at[j * 8 + kc * 2 + 1 - h], mine, s, r, pc.partner()))
        return out

    def onward(self, j):
        pc, c = self.pc, self.c
        out = []
        for d, dl in enumerate((1, -1)):
            origin = rem4(pc.k[c] - dl + RING)
            s, r = self.sems(j, 7 + d, 7 + pc.core)
            out.append(remote(self.transit.at[d, j], self.land.at[j * 8 + origin * 2 + pc.core], s, r, pc.peer(c, dl, d)))
        return out

    def wait_transit(self, j):
        for d, dl in enumerate((1, -1)):
            s, r = self.sems(j, 5 + d, 5 + d)
            remote(self.transit.at[d, j], self.transit.at[d, j], s, r, self.pc.peer(self.c, dl)).wait_recv()

    def wait_land(self, j):
        pc, c = self.pc, self.c
        kc, h = pc.k[c], pc.core
        other = pc.partner()

        def arrived(n, origin, core):
            s, r = self.sems(j, 0, n)
            block = self.land.at[j * 8 + origin * 2 + core]
            remote(block, block, s, r, other).wait_recv()

        arrived(0, kc, 1 - h)
        for d, dl in enumerate((1, -1)):
            for core in range(2):
                arrived(1 + d * 2 + core, rem4(kc - dl + RING), core)
        for core in range(2):
            arrived(7 + core, rem4(kc + 2), core)

    def wait_sent(self, j):
        for cp in self.first(j) + self.onward(j):
            cp.wait_send()


def slots_of(rows, ids):
    return [ids[n:n + 1, :] == rows for n in range(ids.shape[0])]


def expert_kernel(dims, tok, meta, wg, wu, wd, y0, y1, y2, ma, t0, t1, t2, mm, s0, s1, s2, l0, l1, l2, r0, r1, r2, x, hid,
                  o0, o1, o2, vg, vu, vd, send, recv, here):
    widths, starts = dims
    pc = Place()
    ys, ts, ss, ls, rs, os = (y0, y1, y2), (t0, t1, t2), (s0, s1, s2), (l0, l1, l2), (r0, r1, r2), (o0, o1, o2)
    axes = [(p, (p + 1) % 3, (p + 2) % 3) for p in range(3)]
    k = pc.k
    half = tok.shape[0] // 2
    top_k = meta.shape[0] // 2
    sent = []

    loads = []
    for p, (a, b, c) in enumerate(axes):
        loads.append(pltpu.make_async_copy(tok.at[:, pl.ds(starts[p], widths[p])], ts[p].at[k[b], k[a]], here.at[p]))
        loads.append(pltpu.make_async_copy(meta, mm.at[p, k[b], k[a]], here.at[3 + p]))
    weights = [pltpu.make_async_copy(src.at[0], dst, here.at[6 + n]) for n, (src, dst) in enumerate(((wg, vg), (wu, vu), (wd, vd)))]
    for cp in loads:
        cp.start()
    pc.barrier()
    for cp in loads:
        cp.wait()
    for cp in weights:
        cp.start()

    def push(p, n, ref, dev):
        cp = remote(ref, ref, send.at[p, n], recv.at[p, n], dev)
        cp.start()
        sent.append(cp)

    def got(p, n, ref):
        remote(ref, ref, send.at[p, n], recv.at[p, n], pc.partner()).wait_recv()

    def blk(p, da, db):
        a, b, c = axes[p]
        return ts[p].at[rem4(k[b] + db), rem4(k[a] + da)]

    def part_of(ref, d):
        return ref.at[pl.ds(d * half, half)]

    def up(p, ax):
        return pc.peer(axes[p][ax], 1)

    def down(p, ax):
        return pc.peer(axes[p][ax], -1)

    def along_b(p, da):
        push(p, 7 + da * 3, blk(p, da, 0), up(p, 1))
        push(p, 8 + da * 3, blk(p, da, 0), down(p, 1))

    def meta_of(p, da):
        a, b, c = axes[p]
        return mm.at[p, k[b], rem4(k[a] + da)]

    def meta_row(p, db):
        return mm.at[p, rem4(k[axes[p][1]] + db)]

    for p in range(3):
        push(p, 4, meta_of(p, 0), up(p, 0))
        push(p, 5, meta_of(p, 0), down(p, 0))
        push(p, 0, blk(p, 0, 0), up(p, 0))
        push(p, 1, blk(p, 0, 0), down(p, 0))
    for p in range(3):
        along_b(p, 0)
    for p in range(3):
        got(p, 4, meta_of(p, 3))
        push(p, 6, meta_of(p, 3), up(p, 0))
        got(p, 5, meta_of(p, 1))
    for p in range(3):
        got(p, 0, blk(p, 3, 0))
        push(p, 2, part_of(blk(p, 3, 0), 0), up(p, 0))
        got(p, 1, blk(p, 1, 0))
        push(p, 3, part_of(blk(p, 1, 0), 1), down(p, 0))
    for p in range(3):
        got(p, 6, meta_of(p, 2))
        push(p, 19, meta_row(p, 0), up(p, 1))
        push(p, 20, meta_row(p, 0), down(p, 1))
        along_b(p, 3)
        along_b(p, 1)
    for p in range(3):
        got(p, 7, blk(p, 0, 3))
        push(p, 9, blk(p, 0, 3), up(p, 1))
    for p in range(3):
        got(p, 2, part_of(blk(p, 2, 0), 0))
        got(p, 3, part_of(blk(p, 2, 0), 1))
        along_b(p, 2)
    keep = [pltpu.make_async_copy(mm.at[p, k[axes[p][1]]], ma.at[p], here.at[9 + p]) for p in range(3)]
    for cp in keep:
        cp.start()
    for p in range(3):
        got(p, 19, meta_row(p, 3))
        push(p, 21, meta_row(p, 3), up(p, 1))
    for da in (3, 1):
        for p in range(3):
            got(p, 8 + da * 3, blk(p, da, 1))
            push(p, 9 + da * 3, blk(p, da, 1), down(p, 1))
    for p in range(3):
        got(p, 7 + 6, blk(p, 2, 3))
        push(p, 9 + 6, blk(p, 2, 3), up(p, 1))
    for p in range(3):
        got(p, 20, meta_row(p, 1))
        got(p, 21, meta_row(p, 2))
        got(p, 8, blk(p, 0, 1))
        got(p, 8 + 6, blk(p, 2, 1))
        for da in (3, 1):
            got(p, 7 + da * 3, blk(p, da, 3))
        for da in (0, 3, 1, 2):
            got(p, 9 + da * 3, blk(p, da, 2))

    lines = [Exchange(pc, axes[p][2], ss[p], ls[p], rs[p], send.at[p], recv.at[p], 22) for p in range(3)]
    row = lax.broadcasted_iota(jnp.int32, (8 * SLOTS, tok.shape[0]), 0)

    def picks(j):
        for p, (a, b, c) in enumerate(axes):
            first = SLOTS * (pc.me - k[c] * STRIDE[c] - pc.core)
            rows = (first + (row >> 5) * (SLOTS * STRIDE[c]) + (row & 31)).astype(F32)

            @pl.loop(0, RING)
            def _(bb):
                aa = rem4(j + 2 * RING - k[c] - bb)
                ids = mm[p, bb, aa][:top_k]
                hot = sum(jnp.where(hit, 1.0, 0.0) for hit in slots_of(rows, ids)).astype(BF16)
                got_rows = jnp.dot(hot, ts[p][bb, aa], preferred_element_type=F32).astype(BF16)
                ss[p][pl.ds(j * 8, 8), bb] = got_rows.reshape(8, SLOTS, widths[p])

            own = j * 8 + k[c] * 2 + pc.core
            ls[p][own] = ss[p][own]

    def places(j, zy, core):
        z, yy = lax.div(zy, RING), rem4(zy)
        xx = rem4(j + 2 * RING - z - yy)
        return [(j * 8 + cc * 2 + core, bb) for cc, bb in ((xx, yy), (z, xx), (yy, z))]

    def ffn(j):
        @pl.loop(0, RING * RING)
        def _(zy):
            for core in range(2):
                for p, (cc, bb) in enumerate(places(j, zy, core)):
                    x[pl.ds(pl.multiple_of((zy * 2 + core) * SLOTS, SLOTS), SLOTS), pl.ds(starts[p], widths[p])] = ls[p][cc, bb]

        @pl.loop(0, hid.shape[1] // 256)
        def _(n):
            cols = pl.ds(pl.multiple_of(n * 256, 256), 256)
            g = jnp.dot(x[...], vg[:, cols], preferred_element_type=F32)
            u = jnp.dot(x[...], vu[:, cols], preferred_element_type=F32)
            hid[:, cols] = (g * jax.nn.sigmoid(g) * u).astype(BF16)

        @pl.loop(0, x.shape[1] // 256)
        def _(n):
            cols = pl.ds(pl.multiple_of(n * 256, 256), 256)
            x[:, cols] = jnp.dot(hid[...], vd[:, cols], preferred_element_type=F32).astype(BF16)

        @pl.loop(0, RING * RING)
        def _(zy):
            for core in range(2):
                for p, (cc, bb) in enumerate(places(j, zy, core)):
                    os[p][cc, bb] = x[pl.ds(pl.multiple_of((zy * 2 + core) * SLOTS, SLOTS), SLOTS), pl.ds(starts[p], widths[p])]

    def stores(j):
        return [pltpu.make_async_copy(os[p].at[pl.ds(j * 8, 8)], ys[p].at[pl.ds(j * 8, 8)], here.at[12 + p * RING + j]) for p in range(3)]

    for cp in weights:
        cp.wait()

    @pl.loop(0, RING + 2)
    def _(i):
        @pl.when(i < RING)
        def _():
            picks(i)
            for line in lines:
                for cp in line.first(i):
                    cp.start()

        @pl.when((i >= 1) & (i < RING + 1))
        def _():
            for line in lines:
                line.wait_transit(i - 1)
                for cp in line.onward(i - 1):
                    cp.start()

        @pl.when(i >= 2)
        def _():
            for line in lines:
                line.wait_land(i - 2)
            ffn(i - 2)
            for cp in stores(i - 2):
                cp.start()

    for cp in keep:
        cp.wait()
    for cp in sent:
        cp.wait_send()

    @pl.loop(0, RING)
    def _(j):
        for line in lines:
            line.wait_sent(j)
        for cp in stores(j):
            cp.wait()


def return_kernel(dims, y0, y1, y2, ma, out, l0, l1, l2, r0, r1, r2, m0, m1, m2, b0, b1, b2, a0, a1, a2, f0, f1, f2, g0, g1, g2,
                  z0, z1, z2, hot, send, recv, here):
    widths, starts = dims
    pc = Place()
    ys, ls, rs, ms, bs, sums = (y0, y1, y2), (l0, l1, l2), (r0, r1, r2), (m0, m1, m2), (b0, b1, b2), (a0, a1, a2)
    fars, nears, zs = (f0, f1, f2), (g0, g1, g2), (z0, z1, z2)
    axes = [(p, (p + 1) % 3, (p + 2) % 3) for p in range(3)]
    k = pc.k
    toks = out.shape[0]
    half = toks // 2
    top_k = ma.shape[2] // 2
    lines = [Exchange(pc, axes[p][2], ys[p], ls[p], rs[p], send.at[p], recv.at[p], 0) for p in range(3)]

    def own(p, j):
        at = j * 8 + k[axes[p][2]] * 2 + pc.core
        return pltpu.make_async_copy(ys[p].at[at], ls[p].at[at], here.at[p, j])

    def sems(p, j, n):
        at = 36 + j * 6 + n
        return send.at[p, at], recv.at[p, at]

    def second(p, j):
        b = axes[p][1]
        cps = []
        for d, dl in enumerate((1, -1)):
            far = ls[p].at[pl.ds(j * 8 + d * 4, 4), rem4(k[b] + 2)]
            cps.append(remote(far, bs[p].at[d, j], *sems(p, j, 2 + d), pc.peer(b, dl)))
        for d, dl in enumerate((1, -1)):
            near = ls[p].at[pl.ds(j * 8, 8), rem4(k[b] + dl + RING)]
            cps.append(remote(near, ms[p].at[j * RING + k[b]], *sems(p, j, d), pc.peer(b, dl)))
        return cps

    def far_rows(p, j, d, origin):
        return ms[p].at[j * RING + origin, pl.ds(d * 4, 4)]

    def second_on(p, j):
        b = axes[p][1]
        return [
            remote(bs[p].at[d, j], far_rows(p, j, d, rem4(k[b] - dl + RING)), *sems(p, j, 4 + d), pc.peer(b, dl))
            for d, dl in enumerate((1, -1))
        ]

    def got(ref, pair):
        remote(ref, ref, *pair, pc.partner()).wait_recv()

    row = lax.broadcasted_iota(jnp.int32, (8 * SLOTS, toks), 0)

    def combine(p, j):
        a, b, c = axes[p]
        src = rem4(j + 2 * RING - k[c] - k[b])
        first = SLOTS * (pc.me - k[b] * STRIDE[b] - k[c] * STRIDE[c] - pc.core)
        info = ma[p, src]
        rows = first + (row >> 5) * (SLOTS * STRIDE[c]) + (row & 31)

        @pl.loop(0, RING)
        def _(bb):
            hits = slots_of((rows + bb * (SLOTS * STRIDE[b])).astype(F32), info[:top_k])
            pick = sum(jnp.where(hit, 1.0, 0.0) for hit in hits)
            gate = sum(jnp.where(hit, info[top_k + n:top_k + n + 1, :], 0.0) for n, hit in enumerate(hits))
            gate = jnp.sum(gate, axis=1, keepdims=True)
            at = pl.ds(pl.multiple_of(bb * 8 * SLOTS, 8 * SLOTS), 8 * SLOTS)
            hot[p, at] = pick.astype(BF16)
            zs[p][at] = (ms[p][j * RING + bb].reshape(8 * SLOTS, widths[p]).astype(F32) * gate).astype(BF16)

        sums[p][src] = lax.dot_general(hot[p], zs[p][...], (((0,), (0,)), ((), ())), preferred_element_type=F32)

    pc.barrier()

    @pl.loop(0, 2 * RING)
    def _(i):
        @pl.when(i < RING)
        def _():
            for p in range(3):
                own(p, i).start()
                for cp in lines[p].first(i):
                    cp.start()

        @pl.when((i >= 1) & (i < RING + 1))
        def _():
            for p in range(3):
                lines[p].wait_transit(i - 1)
                for cp in lines[p].onward(i - 1):
                    cp.start()

        @pl.when((i >= 2) & (i < RING + 2))
        def _():
            j = i - 2
            for p in range(3):
                own(p, j).wait()
                lines[p].wait_land(j)
                for cp in second(p, j):
                    cp.start()
                b = axes[p][1]
                ms[p][j * RING + k[b]] = ls[p][pl.ds(j * 8, 8), k[b]]

        @pl.when((i >= 3) & (i < RING + 3))
        def _():
            j = i - 3
            for p in range(3):
                for d in range(2):
                    got(bs[p].at[d, j], sems(p, j, 2 + d))
                for cp in second_on(p, j):
                    cp.start()

        @pl.when(i >= RING)
        def _():
            j = i - RING
            for p in range(3):
                b = axes[p][1]
                for d, dl in enumerate((1, -1)):
                    got(ms[p].at[j * RING + rem4(k[b] - dl + RING)], sems(p, j, d))
                    got(far_rows(p, j, d, rem4(k[b] + 2)), sems(p, j, 4 + d))
                combine(p, j)

    def at_sem(p, n):
        return send.at[p, 60 + n], recv.at[p, 60 + n]

    tail = []
    for p in range(3):
        a = axes[p][0]
        for d, dl in enumerate((1, -1)):
            piece = sums[p].at[rem4(k[a] + 2), pl.ds(d * half, half)]
            cp = remote(piece, fars[p].at[d], *at_sem(p, d), pc.peer(a, dl))
            cp.start()
            tail.append(cp)
    for p in range(3):
        a = axes[p][0]
        for d, dl in enumerate((1, -1)):
            got(fars[p].at[d], at_sem(p, d))
            near = rem4(k[a] + dl + RING)
            rows = pl.ds(d * half, half)
            sums[p][near, rows] = sums[p][near, rows] + fars[p][d]
            cp = remote(sums[p].at[near], nears[p].at[d], *at_sem(p, 2 + d), pc.peer(a, dl))
            cp.start()
            tail.append(cp)
    for p in range(3):
        a = axes[p][0]
        for d in range(2):
            got(nears[p].at[d], at_sem(p, 2 + d))
        out[:, pl.ds(starts[p], widths[p])] = (sums[p][k[a]] + nears[p][0] + nears[p][1]).astype(out.dtype)
    for cp in tail:
        cp.wait_send()

    @pl.loop(0, RING)
    def _(j):
        for p in range(3):
            lines[p].wait_sent(j)
            for cp in second(p, j) + second_on(p, j):
                cp.wait_send()


def solution(mesh):
    row_spec = P(("data", "expert"), None)
    weight_spec = P("expert", None, None)
    any_spec = pl.BlockSpec(memory_space=pl.ANY)
    vmem_spec = pl.BlockSpec(memory_space=pltpu.VMEM)

    def device_layer(tokens, expert_ids, gate_wts, dev_slot, exp_slot, w_gate, w_up, w_down):
        toks, top_k = expert_ids.shape
        d_model, d_ff = w_gate.shape[1:]
        tiles = d_model // 128
        widths = [128 * (tiles - 2 * (tiles // 3)), 128 * (tiles // 3), 128 * (tiles // 3)]
        starts = [0, widths[0], widths[0] + widths[1]]
        dims = (widths, starts)
        kept = (dev_slot >= 0) & (exp_slot >= 0)
        dest = jnp.where(kept, expert_ids * SLOTS + dev_slot, -1).astype(F32)
        gate_bf = lax.reduce_precision(gate_wts, 8, 7)
        meta = jnp.concatenate([dest.T, gate_bf.T], axis=0)
        n_blocks = 2 * RING * RING

        def bufs(*lead, dtype=BF16):
            return [pltpu.VMEM((*lead, w), dtype) for w in widths]

        blocks = [jax.ShapeDtypeStruct((n_blocks, RING, SLOTS, w), BF16) for w in widths]
        *ys, ma = pl.pallas_call(
            lambda *refs: expert_kernel(dims, *refs),
            out_shape=(*blocks, jax.ShapeDtypeStruct((3, RING, 2 * top_k, toks), F32)),
            in_specs=[any_spec] * 5,
            out_specs=(any_spec,) * 4,
            scratch_shapes=[
                *bufs(RING, RING, toks),
                pltpu.VMEM((3, RING, RING, 2 * top_k, toks), F32),
                *bufs(n_blocks, RING, SLOTS),
                *bufs(n_blocks, RING, SLOTS),
                *bufs(2, RING, RING, SLOTS),
                pltpu.VMEM((n_blocks * SLOTS, d_model), BF16),
                pltpu.VMEM((n_blocks * SLOTS, d_ff), BF16),
                *bufs(n_blocks, RING, SLOTS),
                pltpu.VMEM((d_model, d_ff), BF16),
                pltpu.VMEM((d_model, d_ff), BF16),
                pltpu.VMEM((d_ff, d_model), BF16),
                pltpu.SemaphoreType.DMA((3, 58)),
                pltpu.SemaphoreType.DMA((3, 58)),
                pltpu.SemaphoreType.DMA((24,)),
            ],
            compiler_params=pltpu.CompilerParams(collective_id=0, has_side_effects=True, vmem_limit_bytes=VMEM_CAP),
            name="dispatch_ffn",
        )(tokens, meta, w_gate, w_up, w_down)
        return pl.pallas_call(
            lambda *refs: return_kernel(dims, *refs),
            out_shape=jax.ShapeDtypeStruct((toks, d_model), BF16),
            in_specs=[any_spec] * 3 + [vmem_spec],
            out_specs=vmem_spec,
            scratch_shapes=[
                *bufs(n_blocks, RING, SLOTS),
                *bufs(2, RING, RING, SLOTS),
                *bufs(RING * RING, 8, SLOTS),
                *bufs(2, RING, RING, SLOTS),
                *bufs(RING, toks, dtype=F32),
                *bufs(2, toks // 2, dtype=F32),
                *bufs(2, toks, dtype=F32),
                *bufs(n_blocks * SLOTS),
                pltpu.VMEM((3, n_blocks * SLOTS, toks), BF16),
                pltpu.SemaphoreType.DMA((3, 64)),
                pltpu.SemaphoreType.DMA((3, 64)),
                pltpu.SemaphoreType.DMA((3, 4)),
            ],
            compiler_params=pltpu.CompilerParams(collective_id=1, has_side_effects=True, vmem_limit_bytes=VMEM_CAP),
            name="combine_return",
        )(*ys, ma)

    def moe_layer(*args):
        return jax.shard_map(device_layer, mesh=mesh, in_specs=(row_spec,) * 5 + (weight_spec,) * 3, out_specs=row_spec, check_vma=False)(*args)

    return moe_layer
```

```python
import jax
import jax.numpy as jnp
from jax import lax
from jax.experimental import pallas as pl
from jax.experimental.pallas import tpu as pltpu
from jax.sharding import PartitionSpec as P

STRIDE = (32, 8, 2)
RING = 4
SLOTS = 16
STEPS = (2, 1, -1)
VMEM_CAP = 67043328
BF16 = jnp.bfloat16
F32 = jnp.float32


def rem4(v):
    return lax.rem(v, RING)


class Place:
    def __init__(self):
        self.me = lax.axis_index("expert")
        self.core = lax.rem(self.me, 2)
        self.k = [rem4(lax.div(self.me, s)) for s in STRIDE]

    def peer(self, axis, delta, core=None):
        there = rem4(self.k[axis] + delta + RING)
        dev = self.me + (there - self.k[axis]) * STRIDE[axis]
        return dev if core is None else dev + core - self.core

    def partner(self):
        return self.me + 1 - 2 * self.core

    def barrier(self):
        sem = pltpu.get_barrier_semaphore()
        peers = [self.peer(ax, dl, c) for ax in range(3) for dl in STEPS for c in (0, 1)] + [self.partner()]
        for dev in peers:
            pl.semaphore_signal(sem, inc=1, device_id={"expert": dev}, device_id_type=pl.DeviceIdType.MESH)
        pl.semaphore_wait(sem, len(peers))


def remote(src, dst, send, recv, dev):
    return pltpu.make_async_remote_copy(
        src_ref=src, dst_ref=dst, send_sem=send, recv_sem=recv, device_id={"expert": dev}, device_id_type=pl.DeviceIdType.MESH
    )


class Exchange:
    def __init__(self, pc, c, block, land, send, recv, base):
        self.pc, self.c, self.block, self.land = pc, c, block, land
        self.send, self.recv, self.base = send, recv, base

    def own(self, j):
        return j * 8 + self.pc.k[self.c] * 2 + self.pc.core

    def sends(self, j):
        pc, c = self.pc, self.c
        at = self.base + j * 7
        mine = self.land.at[self.own(j)]
        out = []
        for n, dl in enumerate(STEPS):
            there = rem4(pc.k[c] + dl + RING)
            for core in range(2):
                sems = self.send.at[at + n * 2 + core], self.recv.at[at + n * 2 + pc.core]
                out.append(remote(self.block(j * 8 + there * 2 + core), mine, *sems, pc.peer(c, dl, core)))
        sems = self.send.at[at + 6], self.recv.at[at + 6]
        out.append(remote(self.block(j * 8 + pc.k[c] * 2 + 1 - pc.core), mine, *sems, pc.partner()))
        return out

    def wait_land(self, j):
        pc, c = self.pc, self.c
        at = self.base + j * 7

        def arrived(n, origin, core):
            block = self.land.at[j * 8 + origin * 2 + core]
            remote(block, block, self.send.at[at], self.recv.at[at + n], pc.partner()).wait_recv()

        arrived(6, pc.k[c], 1 - pc.core)
        for n, dl in enumerate(STEPS):
            for core in range(2):
                arrived(n * 2 + core, rem4(pc.k[c] - dl + RING), core)


def slots_of(rows, ids):
    return [ids[n:n + 1, :] == rows for n in range(ids.shape[0])]


SEM_B = 10
SEM_C = 22
SEM_R = SEM_C + 28
SEM_S = SEM_R + 28
SEM_A = SEM_S + 12
N_SEMS = SEM_A + 6


def layer_kernel(dims, tok, meta, wg, wu, wd, out, t0, t1, t2, mm, s0, s1, s2, l0, l1, l2, x, hid, vg, vu, vd, c0, c1, c2,
                 m0, m1, m2, a0, a1, a2, f0, f1, f2, g0, g1, g2, hot, send, recv, here):
    widths, starts = dims
    pc = Place()
    ts, ss, ls, cs, ms, sums = (t0, t1, t2), (s0, s1, s2), (l0, l1, l2), (c0, c1, c2), (m0, m1, m2), (a0, a1, a2)
    fars, nears = (f0, f1, f2), (g0, g1, g2)
    axes = [(p, (p + 1) % 3, (p + 2) % 3) for p in range(3)]
    k = pc.k
    toks = mm.shape[-1]
    top_k = meta.shape[0] // 2
    half = toks // 2
    sent = []

    def spot(p, da, db):
        a, b, c = axes[p]
        return rem4(k[b] + db) * RING + rem4(k[a] + da)

    def blk(p, da, db):
        return ts[p].at[pl.ds(spot(p, da, db) * 8, 8)]

    def half_blk(p, da, db, d):
        return ts[p].at[pl.ds(spot(p, da, db) * 8 + d * 4, 4)]

    loads = []
    for p, (a, b, c) in enumerate(axes):
        loads.append(pltpu.make_async_copy(tok.at[:, :, pl.ds(starts[p], widths[p])], blk(p, 0, 0), here.at[p]))
        loads.append(pltpu.make_async_copy(meta, mm.at[p, k[b], k[a]], here.at[3 + p]))
    weights = [pltpu.make_async_copy(src.at[0], dst, here.at[6 + n]) for n, (src, dst) in enumerate(((wg, vg), (wu, vu), (wd, vd)))]
    for cp in loads:
        cp.start()
    with jax.named_scope("barrier"):
        pc.barrier()
    for cp in loads:
        cp.wait()

    def push(p, n, ref, dev):
        cp = remote(ref, ref, send.at[p, n], recv.at[p, n], dev)
        cp.start()
        sent.append(cp)

    def got(p, n, ref):
        remote(ref, ref, send.at[p, n], recv.at[p, n], pc.partner()).wait_recv()

    def meta_of(p, da):
        return mm.at[p, k[axes[p][1]], rem4(k[axes[p][0]] + da + RING)]

    def meta_row(p, db):
        return mm.at[p, rem4(k[axes[p][1]] + db + RING)]

    def b_sem(da, n):
        return SEM_B + da * 3 + n

    def along_b(p, da):
        push(p, b_sem(da, 0), blk(p, da, 0), pc.peer(axes[p][1], 1))
        push(p, b_sem(da, 1), blk(p, da, 0), pc.peer(axes[p][1], -1))

    def b_low(p, da):
        got(p, b_sem(da, 0), blk(p, da, 3))
        if da in (0, 2):
            push(p, b_sem(da, 2), blk(p, da, 3), pc.peer(axes[p][1], 1))

    def b_high(p, da):
        got(p, b_sem(da, 1), blk(p, da, 1))
        if da in (1, 3):
            push(p, b_sem(da, 2), blk(p, da, 1), pc.peer(axes[p][1], -1))

    def b_far(p, da):
        got(p, b_sem(da, 2), blk(p, da, 2))

    row = lax.broadcasted_iota(jnp.int32, (8 * SLOTS, toks), 0)

    def pick(p, da, db):
        a, b, c = axes[p]
        aa, bb = rem4(k[a] + da), rem4(k[b] + db)
        j = rem4(aa + bb + k[c])
        first = SLOTS * (pc.me - k[c] * STRIDE[c] - pc.core)
        rows = (first + (row >> 5) * (SLOTS * STRIDE[c]) + (row & 31)).astype(F32)
        ids = mm[p, bb, aa][:top_k]
        chosen = sum(jnp.where(hit, 1.0, 0.0) for hit in slots_of(rows, ids)).astype(BF16)
        block = ts[p][pl.ds((bb * RING + aa) * 8, 8)].reshape(toks, widths[p])
        picked = jnp.dot(chosen, block, preferred_element_type=F32).astype(BF16)
        ss[p][pl.ds(j * 8, 8), bb] = picked.reshape(8, SLOTS, widths[p])

    def sides(p, da):
        @pl.loop(0, 2)
        def _(q):
            pick(p, da, 3 - 2 * q)

    for p in range(3):
        for n, dl in enumerate(STEPS):
            push(p, n, meta_of(p, 0), pc.peer(axes[p][0], dl))
        push(p, 6, blk(p, 0, 0), pc.peer(axes[p][0], 1))
        push(p, 7, blk(p, 0, 0), pc.peer(axes[p][0], -1))
    for p in range(3):
        along_b(p, 0)
    for cp in weights:
        cp.start()
    with jax.named_scope("ag_a"):
        for p in range(3):
            got(p, 6, blk(p, 3, 0))
            along_b(p, 3)
            push(p, 8, half_blk(p, 3, 0, 0), pc.peer(axes[p][0], 1))
            got(p, 7, blk(p, 1, 0))
            along_b(p, 1)
            push(p, 9, half_blk(p, 1, 0, 1), pc.peer(axes[p][0], -1))
    with jax.named_scope("ag_meta"):
        for p in range(3):
            for n, dl in enumerate(STEPS):
                got(p, n, meta_of(p, -dl))
            for n, dl in enumerate(STEPS):
                push(p, 3 + n, meta_row(p, 0), pc.peer(axes[p][1], dl))
    with jax.named_scope("ag_b0"):
        for p in range(3):
            b_low(p, 0)
            b_high(p, 0)
    with jax.named_scope("ag_a2"):
        for p in range(3):
            got(p, 8, half_blk(p, 2, 0, 0))
            got(p, 9, half_blk(p, 2, 0, 1))
            along_b(p, 2)
    with jax.named_scope("pick0"):
        for p in range(3):
            @pl.loop(0, RING)
            def _(q):
                pick(p, q, 0)
    for p in range(3):
        for n, dl in enumerate(STEPS):
            got(p, 3 + n, meta_row(p, -dl))
    for da in (3, 1):
        with jax.named_scope("ag_b13"):
            for p in range(3):
                b_low(p, da)
                b_high(p, da)
        with jax.named_scope("pick13"):
            for p in range(3):
                sides(p, 0 if da == 3 else 3)
    with jax.named_scope("ag_b2"):
        for p in range(3):
            b_far(p, 0)
            b_low(p, 2)
    with jax.named_scope("pick2"):
        for p in range(3):
            sides(p, 1)
            pick(p, 0, 2)
    with jax.named_scope("ag_b3"):
        for p in range(3):
            b_high(p, 2)
            b_far(p, 3)
            b_far(p, 1)
    with jax.named_scope("pick3"):
        for p in range(3):
            sides(p, 2)

            @pl.loop(0, 2)
            def _(q):
                pick(p, 1 + 2 * q, 2)
    with jax.named_scope("ag_b4"):
        for p in range(3):
            b_far(p, 2)
            pick(p, 2, 2)

    to_expert = [
        Exchange(pc, axes[p][2], (lambda n, p=p: ss[p].at[n]), ls[p], send.at[p], recv.at[p], SEM_C) for p in range(3)
    ]
    to_source = [
        Exchange(pc, axes[p][2], (lambda n, p=p: ts[p].at[pl.ds(n * RING, RING)]), cs[p], send.at[p], recv.at[p], SEM_R)
        for p in range(3)
    ]

    with jax.named_scope("issue"):
        @pl.loop(0, RING)
        def _(j):
            for p, line in enumerate(to_expert):
                for cp in line.sends(j):
                    cp.start()
                ls[p][line.own(j)] = ss[p][line.own(j)]

    for cp in weights:
        cp.wait()
    for cp in sent:
        cp.wait_send()

    def places(j, zy, core):
        z, yy = lax.div(zy, RING), rem4(zy)
        xx = rem4(j + 2 * RING - z - yy)
        return [(j * 8 + cc * 2 + core, bb) for cc, bb in ((xx, yy), (z, xx), (yy, z))]

    def ffn(j):
        @pl.loop(0, RING * RING)
        def _(zy):
            for core in range(2):
                for p, (at, bb) in enumerate(places(j, zy, core)):
                    x[pl.ds(pl.multiple_of((zy * 2 + core) * SLOTS, SLOTS), SLOTS), pl.ds(starts[p], widths[p])] = ls[p][at, bb]

        @pl.loop(0, hid.shape[1] // 256)
        def _(n):
            cols = pl.ds(pl.multiple_of(n * 256, 256), 256)
            g = jnp.dot(x[...], vg[:, cols], preferred_element_type=F32)
            u = jnp.dot(x[...], vu[:, cols], preferred_element_type=F32)
            hid[:, cols] = (g * jax.nn.sigmoid(g) * u).astype(BF16)

        @pl.loop(0, x.shape[1] // 256)
        def _(n):
            cols = pl.ds(pl.multiple_of(n * 256, 256), 256)
            x[:, cols] = jnp.dot(hid[...], vd[:, cols], preferred_element_type=F32).astype(BF16)

        @pl.loop(0, RING * RING)
        def _(zy):
            for core in range(2):
                for p, (at, bb) in enumerate(places(j, zy, core)):
                    ts[p][at * RING + bb] = x[pl.ds(pl.multiple_of((zy * 2 + core) * SLOTS, SLOTS), SLOTS), pl.ds(starts[p], widths[p])]

    @pl.loop(0, RING)
    def _(j):
        with jax.named_scope("land"):
            for line in to_expert:
                line.wait_land(j)
        with jax.named_scope("ffn"):
            ffn(j)
        with jax.named_scope("send2"):
            for p, line in enumerate(to_source):
                for cp in line.sends(j):
                    cp.start()
                cs[p][line.own(j)] = ts[p][pl.ds(line.own(j) * RING, RING)]

    def second(p, j):
        b = axes[p][1]
        return [
            remote(cs[p].at[pl.ds(j * 8, 8), rem4(k[b] + dl + RING)], ms[p].at[j * RING + k[b]],
                   send.at[p, SEM_S + j * 3 + n], recv.at[p, SEM_S + j * 3 + n], pc.peer(b, dl))
            for n, dl in enumerate(STEPS)
        ]

    @pl.loop(0, RING)
    def _(j):
        with jax.named_scope("land2"):
            for p, line in enumerate(to_source):
                line.wait_land(j)
                for cp in second(p, j):
                    cp.start()
        for p in range(3):
            kb = k[axes[p][1]]
            ms[p][j * RING + kb] = cs[p][pl.ds(j * 8, 8), kb]

    def combine(p, j):
        a, b, c = axes[p]
        src = rem4(j + 2 * RING - k[c] - k[b])
        first = SLOTS * (pc.me - k[b] * STRIDE[b] - k[c] * STRIDE[c] - pc.core)
        info = mm[p, k[b], src]
        rows = first + (row >> 5) * (SLOTS * STRIDE[c]) + (row & 31)
        cols = pl.ds(starts[p], widths[p])

        @pl.loop(0, RING)
        def _(bb):
            hits = slots_of((rows + bb * (SLOTS * STRIDE[b])).astype(F32), info[:top_k])
            chosen = sum(jnp.where(hit, 1.0, 0.0) for hit in hits)
            gate = sum(jnp.where(hit, info[top_k + n:top_k + n + 1, :], 0.0) for n, hit in enumerate(hits))
            gate = jnp.sum(gate, axis=1, keepdims=True)
            at = pl.ds(pl.multiple_of(bb * 8 * SLOTS, 8 * SLOTS), 8 * SLOTS)
            hot[p, at] = chosen.astype(BF16)
            x[at, cols] = (ms[p][j * RING + bb].reshape(8 * SLOTS, widths[p]).astype(F32) * gate).astype(BF16)

        sums[p][src] = lax.dot_general(hot[p], x[:, cols], (((0,), (0,)), ((), ())), preferred_element_type=F32)

    @pl.loop(0, RING)
    def _(j):
        for p in range(3):
            with jax.named_scope("arrive"):
                for n, dl in enumerate(STEPS):
                    got(p, SEM_S + j * 3 + n, ms[p].at[j * RING + rem4(k[axes[p][1]] - dl + RING)])
            with jax.named_scope("combine"):
                combine(p, j)

    tail = []

    def hand(p, n, ref, dst, dl):
        cp = remote(ref, dst, send.at[p, SEM_A + n], recv.at[p, SEM_A + n], pc.peer(axes[p][0], dl))
        cp.start()
        tail.append(cp)

    sides_of = ((0, 1), (1, -1))
    for p in range(3):
        ka = k[axes[p][0]]
        for d, dl in sides_of:
            hand(p, d, sums[p].at[rem4(ka + 2), pl.ds(d * half, half)], fars[p].at[d], dl)
        for d, dl in sides_of:
            rows = pl.ds((1 - d) * half, half)
            hand(p, 2 + d, sums[p].at[rem4(ka + dl + RING), rows], nears[p].at[d, rows], dl)
    with jax.named_scope("rs1"):
        for p in range(3):
            ka = k[axes[p][0]]
            for d, dl in sides_of:
                got(p, SEM_A + d, fars[p].at[d])
                near = rem4(ka + dl + RING)
                rows = pl.ds(d * half, half)
                sums[p][near, rows] = sums[p][near, rows] + fars[p][d]
                hand(p, 4 + d, sums[p].at[near, rows], nears[p].at[d, rows], dl)
    with jax.named_scope("rs2"):
        for p in range(3):
            for d, dl in sides_of:
                got(p, SEM_A + 2 + d, nears[p].at[d, pl.ds((1 - d) * half, half)])
                got(p, SEM_A + 4 + d, nears[p].at[d, pl.ds(d * half, half)])
            out[:, pl.ds(starts[p], widths[p])] = (sums[p][k[axes[p][0]]] + nears[p][0] + nears[p][1]).astype(out.dtype)
    with jax.named_scope("drain"):
        for cp in tail:
            cp.wait_send()

        @pl.loop(0, RING)
        def _(j):
            for p in range(3):
                for cp in to_expert[p].sends(j) + to_source[p].sends(j) + second(p, j):
                    cp.wait_send()


def solution(mesh):
    row_spec = P(("data", "expert"), None)
    weight_spec = P("expert", None, None)
    any_spec = pl.BlockSpec(memory_space=pl.ANY)

    def device_layer(tokens, expert_ids, gate_wts, dev_slot, exp_slot, w_gate, w_up, w_down):
        toks, top_k = expert_ids.shape
        d_model, d_ff = w_gate.shape[1:]
        tiles = d_model // 128
        widths = [128 * (tiles - 2 * (tiles // 3)), 128 * (tiles // 3), 128 * (tiles // 3)]
        starts = [0, widths[0], widths[0] + widths[1]]
        dims = (widths, starts)
        kept = (dev_slot >= 0) & (exp_slot >= 0)
        dest = jnp.where(kept, expert_ids * SLOTS + dev_slot, -1).astype(F32)
        gate_bf = lax.reduce_precision(gate_wts, 8, 7)
        meta = jnp.concatenate([dest.T, gate_bf.T], axis=0)
        n_blocks = 2 * RING * RING

        def bufs(*lead, dtype=BF16):
            return [pltpu.VMEM((*lead, w), dtype) for w in widths]

        return pl.pallas_call(
            lambda *refs: layer_kernel(dims, *refs),
            out_shape=jax.ShapeDtypeStruct((toks, d_model), BF16),
            in_specs=[any_spec] * 5,
            out_specs=pl.BlockSpec(memory_space=pltpu.VMEM),
            scratch_shapes=[
                *bufs(n_blocks * RING, SLOTS),
                pltpu.VMEM((3, RING, RING, 2 * top_k, toks), F32),
                *bufs(n_blocks, RING, SLOTS),
                *bufs(n_blocks, RING, SLOTS),
                pltpu.VMEM((n_blocks * SLOTS, d_model), BF16),
                pltpu.VMEM((n_blocks * SLOTS, d_ff), BF16),
                pltpu.VMEM((d_model, d_ff), BF16),
                pltpu.VMEM((d_model, d_ff), BF16),
                pltpu.VMEM((d_ff, d_model), BF16),
                *bufs(n_blocks, RING, SLOTS),
                *bufs(RING * RING, 8, SLOTS),
                *bufs(RING, toks, dtype=F32),
                *bufs(2, toks // 2, dtype=F32),
                *bufs(2, toks, dtype=F32),
                pltpu.VMEM((3, n_blocks * SLOTS, toks), BF16),
                pltpu.SemaphoreType.DMA((3, N_SEMS)),
                pltpu.SemaphoreType.DMA((3, N_SEMS)),
                pltpu.SemaphoreType.DMA((9,)),
            ],
            compiler_params=pltpu.CompilerParams(collective_id=0, has_side_effects=True, vmem_limit_bytes=VMEM_CAP),
            name="moe_layer",
        )(tokens.reshape(toks // SLOTS, SLOTS, d_model), meta, w_gate, w_up, w_down)

    def moe_layer(*args):
        return jax.shard_map(device_layer, mesh=mesh, in_specs=(row_spec,) * 5 + (weight_spec,) * 3, out_specs=row_spec, check_vma=False)(*args)

    return moe_layer
```

```python
import jax
import jax.numpy as jnp
from jax import lax
from jax.experimental import pallas as pl
from jax.experimental.pallas import tpu as pltpu
from jax.sharding import PartitionSpec as P

STRIDE = (32, 8, 2)
RING = 4
SLOTS = 16
STEPS = (2, 1, -1)
VMEM_CAP = 67043328
BF16 = jnp.bfloat16
F32 = jnp.float32


def rem4(v):
    return lax.rem(v, RING)


class Place:
    def __init__(self):
        self.me = lax.axis_index("expert")
        self.core = lax.rem(self.me, 2)
        self.k = [rem4(lax.div(self.me, s)) for s in STRIDE]

    def peer(self, axis, delta, core=None):
        there = rem4(self.k[axis] + delta + RING)
        dev = self.me + (there - self.k[axis]) * STRIDE[axis]
        return dev if core is None else dev + core - self.core

    def partner(self):
        return self.me + 1 - 2 * self.core

    def greet(self):
        sem = pltpu.get_barrier_semaphore()
        peers = [self.peer(ax, dl, c) for ax in range(3) for dl in STEPS for c in (0, 1)] + [self.partner()]
        self.n_peers = len(peers)
        for dev in peers:
            pl.semaphore_signal(sem, inc=1, device_id={"expert": dev}, device_id_type=pl.DeviceIdType.MESH)

    def meet(self):
        pl.semaphore_wait(pltpu.get_barrier_semaphore(), self.n_peers)


def remote(src, dst, send, recv, dev):
    return pltpu.make_async_remote_copy(
        src_ref=src, dst_ref=dst, send_sem=send, recv_sem=recv, device_id={"expert": dev}, device_id_type=pl.DeviceIdType.MESH
    )


class Exchange:
    def __init__(self, pc, c, block, land, send, recv, base):
        self.pc, self.c, self.block, self.land = pc, c, block, land
        self.send, self.recv, self.base = send, recv, base

    def own(self, j):
        return j * 8 + self.pc.k[self.c] * 2 + self.pc.core

    def sends(self, j):
        pc, c = self.pc, self.c
        at = self.base + j * 7
        mine = self.land.at[self.own(j)]
        out = []
        for n, dl in enumerate(STEPS):
            there = rem4(pc.k[c] + dl + RING)
            for core in range(2):
                sems = self.send.at[at + n * 2 + core], self.recv.at[at + n * 2 + pc.core]
                out.append(remote(self.block(j * 8 + there * 2 + core), mine, *sems, pc.peer(c, dl, core)))
        sems = self.send.at[at + 6], self.recv.at[at + 6]
        out.append(remote(self.block(j * 8 + pc.k[c] * 2 + 1 - pc.core), mine, *sems, pc.partner()))
        return out

    def wait_land(self, j):
        pc, c = self.pc, self.c
        at = self.base + j * 7

        def arrived(n, origin, core):
            block = self.land.at[j * 8 + origin * 2 + core]
            remote(block, block, self.send.at[at], self.recv.at[at + n], pc.partner()).wait_recv()

        arrived(6, pc.k[c], 1 - pc.core)
        for n, dl in enumerate(STEPS):
            for core in range(2):
                arrived(n * 2 + core, rem4(pc.k[c] - dl + RING), core)


def slots_of(rows, ids):
    return [ids[n:n + 1, :] == rows for n in range(ids.shape[0])]


SEM_B = 10
SEM_C = 22
SEM_R = SEM_C + 28
SEM_S = SEM_R + 28
SEM_A = SEM_S + 12
N_SEMS = SEM_A + 6


def layer_kernel(dims, tok, ids, devs, exps, gates, wg, wu, wd, out, t0, t1, t2, mm, s0, s1, s2, l0, l1, l2, x, hid, vg, vu, vd, c0, c1, c2,
                 m0, m1, m2, a0, a1, a2, f0, f1, f2, g0, g1, g2, hot, raw, hot_gate, send, recv, here):
    widths, starts = dims
    pc = Place()
    ts, ss, ls, cs, ms, sums = (t0, t1, t2), (s0, s1, s2), (l0, l1, l2), (c0, c1, c2), (m0, m1, m2), (a0, a1, a2)
    fars, nears = (f0, f1, f2), (g0, g1, g2)
    axes = [(p, (p + 1) % 3, (p + 2) % 3) for p in range(3)]
    back = [axes[(p + 2) % 3] for p in range(3)]
    k = pc.k
    toks = mm.shape[-1]
    top_k = ids.shape[0]
    half = toks // 2
    sent = []

    def spot(p, da, db):
        a, b, c = axes[p]
        return rem4(k[b] + db) * RING + rem4(k[a] + da)

    def blk(p, da, db):
        return ts[p].at[pl.ds(spot(p, da, db) * 8, 8)]

    def half_blk(p, da, db, d):
        return ts[p].at[pl.ds(spot(p, da, db) * 8 + d * 4, 4)]

    loads = [
        pltpu.make_async_copy(tok.at[:, :, pl.ds(starts[p], widths[p])], blk(p, 0, 0), here.at[p]) for p in range(3)
    ]
    routes = [pltpu.make_async_copy(src, raw.at[n], here.at[6 + n]) for n, src in enumerate((ids, devs, exps))]
    routes.append(pltpu.make_async_copy(gates, hot_gate, here.at[9]))
    weights = [pltpu.make_async_copy(src.at[0], dst, here.at[3 + n]) for n, (src, dst) in enumerate(((wg, vg), (wu, vu), (wd, vd)))]
    for cp in routes + loads:
        cp.start()
    with jax.named_scope("barrier"):
        pc.greet()
        for cp in routes:
            cp.wait()
        kept = (raw[1] >= 0) & (raw[2] >= 0)
        dest = jnp.where(kept, raw[0] * SLOTS + raw[1], -1).astype(F32)
        gate_bf = hot_gate[...].astype(BF16).astype(F32)
        for p, (a, b, c) in enumerate(axes):
            mm[p, k[b], k[a], pl.ds(0, top_k)] = dest
            mm[p, k[b], k[a], pl.ds(top_k, top_k)] = gate_bf
        for cp in loads:
            cp.wait()
        pc.meet()

    def push(p, n, ref, dev):
        cp = remote(ref, ref, send.at[p, n], recv.at[p, n], dev)
        cp.start()
        sent.append(cp)

    def got(p, n, ref):
        remote(ref, ref, send.at[p, n], recv.at[p, n], pc.partner()).wait_recv()

    def meta_of(p, da):
        return mm.at[p, k[axes[p][1]], rem4(k[axes[p][0]] + da + RING)]

    def meta_row(p, db):
        return mm.at[p, rem4(k[axes[p][1]] + db + RING)]

    def b_sem(da, n):
        return SEM_B + da * 3 + n

    def along_b(p, da):
        push(p, b_sem(da, 0), blk(p, da, 0), pc.peer(axes[p][1], 1))
        push(p, b_sem(da, 1), blk(p, da, 0), pc.peer(axes[p][1], -1))

    def b_low(p, da):
        got(p, b_sem(da, 0), blk(p, da, 3))
        if da in (0, 2):
            push(p, b_sem(da, 2), blk(p, da, 3), pc.peer(axes[p][1], 1))

    def b_high(p, da):
        got(p, b_sem(da, 1), blk(p, da, 1))
        if da in (1, 3):
            push(p, b_sem(da, 2), blk(p, da, 1), pc.peer(axes[p][1], -1))

    def b_far(p, da):
        got(p, b_sem(da, 2), blk(p, da, 2))

    row = lax.broadcasted_iota(jnp.int32, (8 * SLOTS, toks), 0)

    def pick(p, da, db):
        a, b, c = axes[p]
        aa, bb = rem4(k[a] + da), rem4(k[b] + db)
        j = rem4(aa + bb + k[c])
        first = SLOTS * (pc.me - k[c] * STRIDE[c] - pc.core)
        rows = (first + (row >> 5) * (SLOTS * STRIDE[c]) + (row & 31)).astype(F32)
        ids = mm[p, bb, aa][:top_k]
        chosen = sum(jnp.where(hit, 1.0, 0.0) for hit in slots_of(rows, ids)).astype(BF16)
        block = ts[p][pl.ds((bb * RING + aa) * 8, 8)].reshape(toks, widths[p])
        picked = jnp.dot(chosen, block, preferred_element_type=F32).astype(BF16)
        ss[p][pl.ds(j * 8, 8), bb] = picked.reshape(8, SLOTS, widths[p])

    def sides(p, da):
        @pl.loop(0, 2)
        def _(q):
            pick(p, da, 3 - 2 * q)

    for p in range(3):
        for n, dl in enumerate(STEPS):
            push(p, n, meta_of(p, 0), pc.peer(axes[p][0], dl))
        push(p, 6, blk(p, 0, 0), pc.peer(axes[p][0], 1))
        push(p, 7, blk(p, 0, 0), pc.peer(axes[p][0], -1))
    for p in range(3):
        along_b(p, 0)
    for cp in weights:
        cp.start()
    with jax.named_scope("ag_meta"):
        for p in range(3):
            for n, dl in enumerate(STEPS):
                got(p, n, meta_of(p, -dl))
            for n, dl in enumerate(STEPS):
                push(p, 3 + n, meta_row(p, 0), pc.peer(axes[p][1], dl))
    with jax.named_scope("ag_a"):
        for p in range(3):
            got(p, 6, blk(p, 3, 0))
            push(p, 8, half_blk(p, 3, 0, 0), pc.peer(axes[p][0], 1))
            got(p, 7, blk(p, 1, 0))
            push(p, 9, half_blk(p, 1, 0, 1), pc.peer(axes[p][0], -1))
        for p in range(3):
            along_b(p, 3)
        for p in range(3):
            along_b(p, 1)
    with jax.named_scope("pick0"):
        for p in range(3):
            @pl.loop(0, 3)
            def _(q):
                pick(p, q + lax.div(q, 2), 0)
    with jax.named_scope("ag_a2"):
        for p in range(3):
            got(p, 8, half_blk(p, 2, 0, 0))
            got(p, 9, half_blk(p, 2, 0, 1))
            along_b(p, 2)
    with jax.named_scope("ag_b0"):
        for p in range(3):
            b_low(p, 0)
            b_high(p, 0)
    for p in range(3):
        for n, dl in enumerate(STEPS):
            got(p, 3 + n, meta_row(p, -dl))
    with jax.named_scope("pick1"):
        for p in range(3):
            pick(p, 2, 0)
            sides(p, 0)
    for da in (3, 1):
        with jax.named_scope("ag_b13"):
            for p in range(3):
                b_low(p, da)
                b_high(p, da)
        with jax.named_scope("pick13"):
            for p in range(3):
                sides(p, da)
    with jax.named_scope("ag_b2"):
        for p in range(3):
            b_low(p, 2)
            b_high(p, 2)
    with jax.named_scope("pick2"):
        for p in range(3):
            sides(p, 2)
    to_expert = [
        Exchange(pc, axes[p][2], (lambda n, p=p: ss[p].at[n]), ls[p], send.at[p], recv.at[p], SEM_C) for p in range(3)
    ]
    to_source = [
        Exchange(pc, back[p][2], (lambda n, p=p: ts[p].at[pl.ds(n * RING, RING)]), cs[p], send.at[p], recv.at[p], SEM_R)
        for p in range(3)
    ]

    with jax.named_scope("ag_b3"):
        for p in range(3):
            b_far(p, 0)
            b_far(p, 3)
    with jax.named_scope("pick3"):
        for p in range(3):
            @pl.loop(0, 2)
            def _(q):
                pick(p, 3 * q, 2)
    for p in (1, 2, 0):
        with jax.named_scope("ag_b4"):
            b_far(p, 1)
            b_far(p, 2)
        with jax.named_scope("pick4"):
            @pl.loop(0, 2)
            def _(q):
                pick(p, 1 + q, 2)

            line = to_expert[p]

            @pl.loop(0, RING)
            def _(j):
                for cp in line.sends(j):
                    cp.start()
                ls[p][line.own(j)] = ss[p][line.own(j)]

    for cp in weights:
        cp.wait()
    for cp in sent:
        cp.wait_send()

    def places(order, j, zy, core):
        z, yy = lax.div(zy, RING), rem4(zy)
        at = (z, yy, rem4(j + 2 * RING - z - yy))
        return [(j * 8 + at[c] * 2 + core, at[b]) for a, b, c in order]

    def ffn(j):
        @pl.loop(0, RING * RING)
        def _(zy):
            for core in range(2):
                for p, (at, bb) in enumerate(places(axes, j, zy, core)):
                    x[pl.ds(pl.multiple_of((zy * 2 + core) * SLOTS, SLOTS), SLOTS), pl.ds(starts[p], widths[p])] = ls[p][at, bb]

        @pl.loop(0, hid.shape[1] // 256)
        def _(n):
            cols = pl.ds(pl.multiple_of(n * 256, 256), 256)
            g = jnp.dot(x[...], vg[:, cols], preferred_element_type=F32)
            u = jnp.dot(x[...], vu[:, cols], preferred_element_type=F32)
            hid[:, cols] = (g * jax.nn.sigmoid(g) * u).astype(BF16)

        @pl.loop(0, x.shape[1] // 256)
        def _(n):
            cols = pl.ds(pl.multiple_of(n * 256, 256), 256)
            x[:, cols] = jnp.dot(hid[...], vd[:, cols], preferred_element_type=F32).astype(BF16)

        @pl.loop(0, RING * RING)
        def _(zy):
            for core in range(2):
                for p, (at, bb) in enumerate(places(back, j, zy, core)):
                    ts[p][at * RING + bb] = x[pl.ds(pl.multiple_of((zy * 2 + core) * SLOTS, SLOTS), SLOTS), pl.ds(starts[p], widths[p])]

    @pl.loop(0, RING)
    def _(j):
        with jax.named_scope("land"):
            for line in to_expert:
                line.wait_land(j)
        with jax.named_scope("ffn"):
            ffn(j)
        with jax.named_scope("send2"):
            for p, line in enumerate(to_source):
                for cp in line.sends(j):
                    cp.start()
                cs[p][line.own(j)] = ts[p][pl.ds(line.own(j) * RING, RING)]

    def second(p, j):
        b = back[p][1]
        return [
            remote(cs[p].at[pl.ds(j * 8, 8), rem4(k[b] + dl + RING)], ms[p].at[j * RING + k[b]],
                   send.at[p, SEM_S + j * 3 + n], recv.at[p, SEM_S + j * 3 + n], pc.peer(b, dl))
            for n, dl in enumerate(STEPS)
        ]

    @pl.loop(0, RING)
    def _(j):
        with jax.named_scope("land2"):
            for p, line in enumerate(to_source):
                line.wait_land(j)
                for cp in second(p, j):
                    cp.start()
        for p in range(3):
            kb = k[back[p][1]]
            ms[p][j * RING + kb] = cs[p][pl.ds(j * 8, 8), kb]

    def combine(p, j):
        a, b, c = back[p]
        src = rem4(j + 2 * RING - k[c] - k[b])
        first = SLOTS * (pc.me - k[b] * STRIDE[b] - k[c] * STRIDE[c] - pc.core)
        info = mm[(p + 2) % 3, k[b], src]
        rows = first + (row >> 5) * (SLOTS * STRIDE[c]) + (row & 31)
        cols = pl.ds(starts[p], widths[p])

        @pl.loop(0, RING)
        def _(bb):
            hits = slots_of((rows + bb * (SLOTS * STRIDE[b])).astype(F32), info[:top_k])
            chosen = sum(jnp.where(hit, 1.0, 0.0) for hit in hits)
            gate = sum(jnp.where(hit, info[top_k + n:top_k + n + 1, :], 0.0) for n, hit in enumerate(hits))
            gate = jnp.sum(gate, axis=1, keepdims=True)
            at = pl.ds(pl.multiple_of(bb * 8 * SLOTS, 8 * SLOTS), 8 * SLOTS)
            hot[p, at] = chosen.astype(BF16)
            x[at, cols] = (ms[p][j * RING + bb].reshape(8 * SLOTS, widths[p]).astype(F32) * gate).astype(BF16)

        sums[p][src] = lax.dot_general(hot[p], x[:, cols], (((0,), (0,)), ((), ())), preferred_element_type=F32)

    def gathered(p, j):
        with jax.named_scope("arrive"):
            for n, dl in enumerate(STEPS):
                got(p, SEM_S + j * 3 + n, ms[p].at[j * RING + rem4(k[back[p][1]] - dl + RING)])
        with jax.named_scope("combine"):
            combine(p, j)

    @pl.loop(0, RING - 1)
    def _(j):
        for p in range(3):
            gathered(p, j)

    tail = []

    def hand(p, n, ref, dst, dl):
        cp = remote(ref, dst, send.at[p, SEM_A + n], recv.at[p, SEM_A + n], pc.peer(back[p][0], dl))
        cp.start()
        tail.append(cp)

    sides_of = ((0, 1), (1, -1))
    for p in range(3):
        gathered(p, RING - 1)
        ka = k[back[p][0]]
        for d, dl in sides_of:
            hand(p, d, sums[p].at[rem4(ka + 2), pl.ds(d * half, half)], fars[p].at[d], dl)
        for d, dl in sides_of:
            rows = pl.ds((1 - d) * half, half)
            hand(p, 2 + d, sums[p].at[rem4(ka + dl + RING), rows], nears[p].at[d, rows], dl)
    with jax.named_scope("rs1"):
        for p in range(3):
            ka = k[back[p][0]]
            for d, dl in sides_of:
                got(p, SEM_A + d, fars[p].at[d])
                near = rem4(ka + dl + RING)
                rows = pl.ds(d * half, half)
                sums[p][near, rows] = sums[p][near, rows] + fars[p][d]
                hand(p, 4 + d, sums[p].at[near, rows], nears[p].at[d, rows], dl)
    with jax.named_scope("rs2"):
        for p in range(3):
            for d, dl in sides_of:
                got(p, SEM_A + 2 + d, nears[p].at[d, pl.ds((1 - d) * half, half)])
                got(p, SEM_A + 4 + d, nears[p].at[d, pl.ds(d * half, half)])
            out[:, pl.ds(starts[p], widths[p])] = sums[p][k[back[p][0]]] + nears[p][0] + nears[p][1]
    with jax.named_scope("drain"):
        for cp in tail:
            cp.wait_send()

        @pl.loop(0, RING)
        def _(j):
            for p in range(3):
                for cp in to_expert[p].sends(j) + to_source[p].sends(j) + second(p, j):
                    cp.wait_send()


def solution(mesh):
    row_spec = P(("data", "expert"), None)
    weight_spec = P("expert", None, None)
    any_spec = pl.BlockSpec(memory_space=pl.ANY)

    def device_layer(tokens, expert_ids, gate_wts, dev_slot, exp_slot, w_gate, w_up, w_down):
        toks, top_k = expert_ids.shape
        d_model, d_ff = w_gate.shape[1:]
        tiles = d_model // 128
        widths = [128 * (tiles - 2 * (tiles // 3)), 128 * (tiles // 3), 128 * (tiles // 3)]
        starts = [0, widths[0], widths[0] + widths[1]]
        dims = (widths, starts)
        n_blocks = 2 * RING * RING

        def bufs(*lead, dtype=BF16):
            return [pltpu.VMEM((*lead, w), dtype) for w in widths]

        summed = pl.pallas_call(
            lambda *refs: layer_kernel(dims, *refs),
            out_shape=jax.ShapeDtypeStruct((toks, d_model), F32),
            in_specs=[any_spec] * 8,
            out_specs=pl.BlockSpec(memory_space=pltpu.VMEM),
            scratch_shapes=[
                *bufs(n_blocks * RING, SLOTS),
                pltpu.VMEM((3, RING, RING, 2 * top_k, toks), F32),
                *bufs(n_blocks, RING, SLOTS),
                *bufs(n_blocks, RING, SLOTS),
                pltpu.VMEM((n_blocks * SLOTS, d_model), BF16),
                pltpu.VMEM((n_blocks * SLOTS, d_ff), BF16),
                pltpu.VMEM((d_model, d_ff), BF16),
                pltpu.VMEM((d_model, d_ff), BF16),
                pltpu.VMEM((d_ff, d_model), BF16),
                *bufs(n_blocks, RING, SLOTS),
                *bufs(RING * RING, 8, SLOTS),
                *bufs(RING, toks, dtype=F32),
                *bufs(2, toks // 2, dtype=F32),
                *bufs(2, toks, dtype=F32),
                pltpu.VMEM((3, n_blocks * SLOTS, toks), BF16),
                pltpu.VMEM((3, top_k, toks), jnp.int32),
                pltpu.VMEM((top_k, toks), F32),
                pltpu.SemaphoreType.DMA((3, N_SEMS)),
                pltpu.SemaphoreType.DMA((3, N_SEMS)),
                pltpu.SemaphoreType.DMA((10,)),
            ],
            compiler_params=pltpu.CompilerParams(collective_id=0, has_side_effects=True, vmem_limit_bytes=VMEM_CAP),
            name="moe_layer",
        )(tokens.reshape(toks // SLOTS, SLOTS, d_model), expert_ids.T, dev_slot.T, exp_slot.T, gate_wts.T, w_gate, w_up, w_down)
        return summed.astype(BF16)

    def moe_layer(*args):
        return jax.shard_map(device_layer, mesh=mesh, in_specs=(row_spec,) * 5 + (weight_spec,) * 3, out_specs=row_spec, check_vma=False)(*args)

    return moe_layer
```

```python
import jax
import jax.numpy as jnp
from jax import lax
from jax.experimental import pallas as pl
from jax.experimental.pallas import tpu as pltpu
from jax.sharding import PartitionSpec as P

STRIDE = (32, 8, 2)
RING = 4
SLOTS = 16
STEPS = (2, 1, -1)
VMEM_CAP = 67043328
BF16 = jnp.bfloat16
F32 = jnp.float32


def rem4(v):
    return lax.rem(v, RING)


class Place:
    def __init__(self):
        self.me = lax.axis_index("expert")
        self.core = lax.rem(self.me, 2)
        self.k = [rem4(lax.div(self.me, s)) for s in STRIDE]

    def peer(self, axis, delta, core=None):
        there = rem4(self.k[axis] + delta + RING)
        dev = self.me + (there - self.k[axis]) * STRIDE[axis]
        return dev if core is None else dev + core - self.core

    def partner(self):
        return self.me + 1 - 2 * self.core

    def greet(self):
        sem = pltpu.get_barrier_semaphore()
        peers = [self.peer(ax, dl, c) for ax in range(3) for dl in STEPS for c in (0, 1)] + [self.partner()]
        self.n_peers = len(peers)
        for dev in peers:
            pl.semaphore_signal(sem, inc=1, device_id={"expert": dev}, device_id_type=pl.DeviceIdType.MESH)

    def meet(self):
        pl.semaphore_wait(pltpu.get_barrier_semaphore(), self.n_peers)


def remote(src, dst, send, recv, dev):
    return pltpu.make_async_remote_copy(
        src_ref=src, dst_ref=dst, send_sem=send, recv_sem=recv, device_id={"expert": dev}, device_id_type=pl.DeviceIdType.MESH
    )


class Exchange:
    def __init__(self, pc, c, block, land, send, recv, base):
        self.pc, self.c, self.block, self.land = pc, c, block, land
        self.send, self.recv, self.base = send, recv, base

    def own(self, j):
        return j * 8 + self.pc.k[self.c] * 2 + self.pc.core

    def sends(self, j):
        pc, c = self.pc, self.c
        sems = self.send, self.recv.at[self.base + j]
        mine = self.land.at[self.own(j)]
        out = []
        for dl in STEPS:
            there = rem4(pc.k[c] + dl + RING)
            for core in range(2):
                out.append(remote(self.block(j * 8 + there * 2 + core), mine, *sems, pc.peer(c, dl, core)))
        out.append(remote(self.block(j * 8 + pc.k[c] * 2 + 1 - pc.core), mine, *sems, pc.partner()))
        return out

    def wait_land(self, j):
        rows = self.land.at[pl.ds(j * 8, 7)]
        remote(rows, rows, self.send, self.recv.at[self.base + j], self.pc.partner()).wait_recv()

    def wait_sent(self):
        rows = self.land.at[pl.ds(0, 7 * RING)]
        remote(rows, rows, self.send, self.recv.at[self.base], self.pc.partner()).wait_send()


def slots_of(rows, ids):
    return [ids[n:n + 1, :] == rows for n in range(ids.shape[0])]


R_META, R_A, R_FAR, R_SIDES, R_ENDS, R_C, R_BACK, R_B, R_SUM, N_RECV = 0, 2, 4, 5, 9, 11, 15, 19, 23, 25
S_META, S_GATHER, S_C, S_BACK, S_B, S_SUM, N_SEND = 0, 2, 3, 4, 5, 6, 7


def layer_kernel(dims, tok, ids, devs, exps, gates, wg, wu, wd, out, t0, t1, t2, mm, s0, s1, s2, l0, l1, l2, x, hid, vg, vu, vd, c0, c1, c2,
                 m0, m1, m2, a0, a1, a2, f0, f1, f2, g0, g1, g2, hot, scale, raw, hot_gate, send, recv, here):
    widths, starts = dims
    pc = Place()
    ts, ss, ls, cs, ms, sums = (t0, t1, t2), (s0, s1, s2), (l0, l1, l2), (c0, c1, c2), (m0, m1, m2), (a0, a1, a2)
    fars, nears = (f0, f1, f2), (g0, g1, g2)
    axes = [(p, (p + 1) % 3, (p + 2) % 3) for p in range(3)]
    back = [axes[(p + 2) % 3] for p in range(3)]
    k = pc.k
    toks = mm.shape[-1]
    top_k = ids.shape[0]
    half = toks // 2

    def spot(p, da, db):
        a, b, c = axes[p]
        return rem4(k[b] + db) * RING + rem4(k[a] + da)

    def blk(p, da, db):
        return ts[p].at[pl.ds(spot(p, da, db) * 8, 8)]

    def half_blk(p, da, db, d):
        return ts[p].at[pl.ds(spot(p, da, db) * 8 + d * 4, 4)]

    loads = [
        pltpu.make_async_copy(tok.at[:, :, pl.ds(starts[p], widths[p])], blk(p, 0, 0), here.at[p]) for p in range(3)
    ]
    routes = [pltpu.make_async_copy(src, raw.at[n], here.at[6 + n]) for n, src in enumerate((ids, devs, exps))]
    routes.append(pltpu.make_async_copy(gates, hot_gate, here.at[9]))
    weights = [pltpu.make_async_copy(src.at[0], dst, here.at[3 + n]) for n, (src, dst) in enumerate(((wg, vg), (wu, vu), (wd, vd)))]
    for cp in routes + loads:
        cp.start()
    with jax.named_scope("barrier"):
        pc.greet()
        for cp in routes:
            cp.wait()
        kept = (raw[1] >= 0) & (raw[2] >= 0)
        dest = jnp.where(kept, raw[0] * SLOTS + raw[1], -1).astype(F32)
        gate_bf = hot_gate[...].astype(BF16).astype(F32)
        for p, (a, b, c) in enumerate(axes):
            mm[p, k[b], k[a], pl.ds(0, top_k)] = dest
            mm[p, k[b], k[a], pl.ds(top_k, top_k)] = gate_bf
        for cp in loads:
            cp.wait()
        pc.meet()

    def push(p, s, r, ref, dev):
        remote(ref, ref, send.at[p, s], recv.at[p, r], dev).start()

    def got(p, r, ref):
        remote(ref, ref, send.at[p, 0], recv.at[p, r], pc.partner()).wait_recv()

    def gone(p, s, ref):
        remote(ref, ref, send.at[p, s], recv.at[p, 0], pc.partner()).wait_send()

    def some(p, n):
        return ts[p].at[pl.ds(0, n * 8)]

    def meta_of(p, da):
        return mm.at[p, k[axes[p][1]], rem4(k[axes[p][0]] + da + RING)]

    def along_b(p, da):
        for dl in (1, -1):
            push(p, S_GATHER, R_SIDES + da, blk(p, da, 0), pc.peer(axes[p][1], dl))

    def b_sides(p, da):
        got(p, R_SIDES + da, some(p, 2))
        dl = 1 if da in (0, 2) else -1
        push(p, S_GATHER, R_ENDS + (da in (1, 2)), blk(p, da, 3 if dl == 1 else 1), pc.peer(axes[p][1], dl))

    def b_ends(p, n):
        got(p, R_ENDS + n, some(p, 2))

    early = rem4(k[0] + k[1] + k[2] + 2)
    row = lax.broadcasted_iota(jnp.int32, (8 * SLOTS, toks), 0)

    def pick(p, da, db):
        a, b, c = axes[p]
        aa, bb = rem4(k[a] + da), rem4(k[b] + db)
        j = rem4(aa + bb + k[c])
        first = SLOTS * (pc.me - k[c] * STRIDE[c] - pc.core)
        rows = (first + (row >> 5) * (SLOTS * STRIDE[c]) + (row & 31)).astype(F32)
        ids = mm[p, bb, aa][:top_k]
        chosen = sum(jnp.where(hit, 1.0, 0.0) for hit in slots_of(rows, ids)).astype(BF16)
        block = ts[p][pl.ds((bb * RING + aa) * 8, 8)].reshape(toks, widths[p])
        picked = jnp.dot(chosen, block, preferred_element_type=F32).astype(BF16)
        ss[p][pl.ds(j * 8, 8), bb] = picked.reshape(8, SLOTS, widths[p])

    def sides(p, da):
        @pl.loop(0, 2)
        def _(q):
            pick(p, da, 3 - 2 * q)

    to_expert = [
        Exchange(pc, axes[p][2], (lambda n, p=p: ss[p].at[n]), ls[p], send.at[p, S_C], recv.at[p], R_C) for p in range(3)
    ]
    def offer(p, j):
        line = to_expert[p]
        for cp in line.sends(j):
            cp.start()
        ls[p][line.own(j)] = ss[p][line.own(j)]

    for p in range(3):
        for dl in STEPS:
            push(p, S_META, R_META, meta_of(p, 0), pc.peer(axes[p][0], dl))
        push(p, S_GATHER, R_A, blk(p, 0, 0), pc.peer(axes[p][0], 1))
        push(p, S_GATHER, R_A + 1, blk(p, 0, 0), pc.peer(axes[p][0], -1))
    for p in range(3):
        along_b(p, 0)
    for cp in weights:
        cp.start()
    with jax.named_scope("ag_meta"):
        for p in range(3):
            got(p, R_META, mm.at[p, 0, pl.ds(0, 3)])
            for dl in STEPS:
                push(p, S_META + 1, R_META + 1, mm.at[p, k[axes[p][1]]], pc.peer(axes[p][1], dl))
    with jax.named_scope("ag_a"):
        for p in range(3):
            got(p, R_A, blk(p, 3, 0))
            push(p, S_GATHER, R_FAR, half_blk(p, 3, 0, 0), pc.peer(axes[p][0], 1))
            got(p, R_A + 1, blk(p, 1, 0))
            push(p, S_GATHER, R_FAR, half_blk(p, 1, 0, 1), pc.peer(axes[p][0], -1))
        for p in range(3):
            along_b(p, 3)
        for p in range(3):
            along_b(p, 1)
    with jax.named_scope("pick0"):
        for p in range(3):
            @pl.loop(0, 3)
            def _(q):
                pick(p, q + lax.div(q, 2), 0)
    with jax.named_scope("ag_a2"):
        for p in range(3):
            got(p, R_FAR, blk(p, 2, 0))
            along_b(p, 2)
    with jax.named_scope("ag_b0"):
        for p in range(3):
            b_sides(p, 0)
    for p in range(3):
        got(p, R_META + 1, mm.at[p, pl.ds(0, 3)])
    with jax.named_scope("pick1"):
        for p in range(3):
            pick(p, 2, 0)
            sides(p, 0)
    for da in (3, 1):
        with jax.named_scope("ag_b13"):
            for p in range(3):
                b_sides(p, da)
        with jax.named_scope("pick13"):
            for p in range(3):
                sides(p, da)
    with jax.named_scope("ag_b2"):
        for p in range(3):
            b_sides(p, 2)
    with jax.named_scope("pick2"):
        for p in range(3):
            sides(p, 2)
    to_source = [
        Exchange(pc, back[p][2], (lambda n, p=p: ts[p].at[pl.ds(n * RING, RING)]), cs[p], send.at[p, S_BACK], recv.at[p], R_BACK)
        for p in range(3)
    ]

    with jax.named_scope("ag_b3"):
        for p in range(3):
            b_ends(p, 0)
    with jax.named_scope("pick3"):
        for p in range(3):
            @pl.loop(0, 2)
            def _(q):
                pick(p, 3 * q, 2)

            offer(p, early)
    for p in (1, 2, 0):
        with jax.named_scope("ag_b4"):
            b_ends(p, 1)
        with jax.named_scope("pick4"):
            @pl.loop(0, 2)
            def _(q):
                pick(p, 1 + q, 2)

            @pl.loop(0, RING - 1)
            def _(q):
                offer(p, q + lax.div(q + RING - early, RING))

    for cp in weights:
        cp.wait()
    for p in range(3):
        gone(p, S_META, mm.at[p, 0, pl.ds(0, 3)])
        gone(p, S_META + 1, mm.at[p, pl.ds(0, 3)])
        gone(p, S_GATHER, some(p, 15))

    def places(order, j, zy, core):
        z, yy = lax.div(zy, RING), rem4(zy)
        at = (z, yy, rem4(j + 2 * RING - z - yy))
        return [(j * 8 + at[c] * 2 + core, at[b]) for a, b, c in order]

    def ffn(j):
        @pl.loop(0, RING * RING)
        def _(zy):
            for core in range(2):
                for p, (at, bb) in enumerate(places(axes, j, zy, core)):
                    x[pl.ds(pl.multiple_of((zy * 2 + core) * SLOTS, SLOTS), SLOTS), pl.ds(starts[p], widths[p])] = ls[p][at, bb]

        g = jnp.dot(x[...], vg[...], preferred_element_type=F32)
        u = jnp.dot(x[...], vu[...], preferred_element_type=F32)
        hid[...] = (g * jax.nn.sigmoid(g) * u).astype(BF16)
        x[...] = jnp.dot(hid[...], vd[...], preferred_element_type=F32).astype(BF16)

        @pl.loop(0, RING * RING)
        def _(zy):
            for core in range(2):
                for p, (at, bb) in enumerate(places(back, j, zy, core)):
                    ts[p][at * RING + bb] = x[pl.ds(pl.multiple_of((zy * 2 + core) * SLOTS, SLOTS), SLOTS), pl.ds(starts[p], widths[p])]

    @pl.loop(0, RING)
    def _(j):
        with jax.named_scope("land"):
            for line in to_expert:
                line.wait_land(j)
        with jax.named_scope("ffn"):
            ffn(j)
        with jax.named_scope("send2"):
            for p, line in enumerate(to_source):
                for cp in line.sends(j):
                    cp.start()
                cs[p][line.own(j)] = ts[p][pl.ds(line.own(j) * RING, RING)]

    def second(p, j):
        b = back[p][1]
        return [
            remote(cs[p].at[pl.ds(j * 8, 8), rem4(k[b] + dl + RING)], ms[p].at[j * RING + k[b]],
                   send.at[p, S_B], recv.at[p, R_B + j], pc.peer(b, dl))
            for dl in STEPS
        ]

    @pl.loop(0, RING)
    def _(j):
        with jax.named_scope("land2"):
            for p, line in enumerate(to_source):
                line.wait_land(j)
                for cp in second(p, j):
                    cp.start()
        for p in range(3):
            kb = k[back[p][1]]
            ms[p][j * RING + kb] = cs[p][pl.ds(j * 8, 8), kb]

    def prepare(p, j):
        a, b, c = back[p]
        src = rem4(j + 2 * RING - k[c] - k[b])
        first = SLOTS * (pc.me - k[b] * STRIDE[b] - k[c] * STRIDE[c] - pc.core)
        info = mm[(p + 2) % 3, k[b], src]
        rows = first + (row >> 5) * (SLOTS * STRIDE[c]) + (row & 31)

        @pl.loop(0, RING)
        def _(bb):
            hits = slots_of((rows + bb * (SLOTS * STRIDE[b])).astype(F32), info[:top_k])
            chosen = sum(jnp.where(hit, 1.0, 0.0) for hit in hits)
            gate = sum(jnp.where(hit, info[top_k + n:top_k + n + 1, :], 0.0) for n, hit in enumerate(hits))
            at = pl.ds(pl.multiple_of(bb * 8 * SLOTS, 8 * SLOTS), 8 * SLOTS)
            hot[p, at] = chosen.astype(BF16)
            scale[p, at] = jnp.sum(gate, axis=1, keepdims=True)

    def combine(p, j):
        a, b, c = back[p]
        src = rem4(j + 2 * RING - k[c] - k[b])
        cols = pl.ds(starts[p], widths[p])

        @pl.loop(0, RING)
        def _(bb):
            at = pl.ds(pl.multiple_of(bb * 8 * SLOTS, 8 * SLOTS), 8 * SLOTS)
            x[at, cols] = (ms[p][j * RING + bb].reshape(8 * SLOTS, widths[p]).astype(F32) * scale[p, at]).astype(BF16)

        sums[p][src] = lax.dot_general(hot[p], x[:, cols], (((0,), (0,)), ((), ())), preferred_element_type=F32)

    def gathered(p, j):
        with jax.named_scope("arrive"):
            got(p, R_B + j, ms[p].at[pl.ds(j * RING, 3)])
        with jax.named_scope("combine"):
            combine(p, j)

    def prepared(j):
        with jax.named_scope("prepare"):
            for p in range(3):
                prepare(p, j)

    @pl.loop(0, RING - 1)
    def _(j):
        prepared(j)
        for p in range(3):
            gathered(p, j)

    prepared(RING - 1)

    def hand(p, r, ref, dst, dl):
        remote(ref, dst, send.at[p, S_SUM], recv.at[p, R_SUM + r], pc.peer(back[p][0], dl)).start()

    sides_of = ((0, 1), (1, -1))
    for p in range(3):
        gathered(p, RING - 1)
        ka = k[back[p][0]]
        for d, dl in sides_of:
            hand(p, 0, sums[p].at[rem4(ka + 2), pl.ds(d * half, half)], fars[p].at[d], dl)
        for d, dl in sides_of:
            rows = pl.ds((1 - d) * half, half)
            hand(p, 1, sums[p].at[rem4(ka + dl + RING), rows], nears[p].at[d, rows], dl)
    with jax.named_scope("rs1"):
        for p in range(3):
            ka = k[back[p][0]]
            got(p, R_SUM, fars[p])
            for d, dl in sides_of:
                near = rem4(ka + dl + RING)
                rows = pl.ds(d * half, half)
                sums[p][near, rows] = sums[p][near, rows] + fars[p][d]
                hand(p, 1, sums[p].at[near, rows], nears[p].at[d, rows], dl)
    with jax.named_scope("rs2"):
        for p in range(3):
            got(p, R_SUM + 1, nears[p])
            out[:, pl.ds(starts[p], widths[p])] = (sums[p][k[back[p][0]]] + nears[p][0] + nears[p][1]).astype(out.dtype)
    with jax.named_scope("drain"):
        for p in range(3):
            to_expert[p].wait_sent()
            to_source[p].wait_sent()
            gone(p, S_B, ms[p].at[pl.ds(0, 3 * RING)])
            gone(p, S_SUM, sums[p].at[pl.ds(0, 3)])


def solution(mesh):
    row_spec = P(("data", "expert"), None)
    weight_spec = P("expert", None, None)
    any_spec = pl.BlockSpec(memory_space=pl.ANY)

    def device_layer(tokens, expert_ids, gate_wts, dev_slot, exp_slot, w_gate, w_up, w_down):
        toks, top_k = expert_ids.shape
        d_model, d_ff = w_gate.shape[1:]
        tiles = d_model // 128
        widths = [128 * (tiles - 2 * (tiles // 3)), 128 * (tiles // 3), 128 * (tiles // 3)]
        starts = [0, widths[0], widths[0] + widths[1]]
        dims = (widths, starts)
        n_blocks = 2 * RING * RING

        def bufs(*lead, dtype=BF16):
            return [pltpu.VMEM((*lead, w), dtype) for w in widths]

        summed = pl.pallas_call(
            lambda *refs: layer_kernel(dims, *refs),
            out_shape=jax.ShapeDtypeStruct((toks, d_model), BF16),
            in_specs=[any_spec] * 8,
            out_specs=pl.BlockSpec(memory_space=pltpu.VMEM),
            scratch_shapes=[
                *bufs(n_blocks * RING, SLOTS),
                pltpu.VMEM((3, RING, RING, 2 * top_k, toks), F32),
                *bufs(n_blocks, RING, SLOTS),
                *bufs(n_blocks, RING, SLOTS),
                pltpu.VMEM((n_blocks * SLOTS, d_model), BF16),
                pltpu.VMEM((n_blocks * SLOTS, d_ff), BF16),
                pltpu.VMEM((d_model, d_ff), BF16),
                pltpu.VMEM((d_model, d_ff), BF16),
                pltpu.VMEM((d_ff, d_model), BF16),
                *bufs(n_blocks, RING, SLOTS),
                *bufs(RING * RING, 8, SLOTS),
                *bufs(RING, toks, dtype=F32),
                *bufs(2, toks // 2, dtype=F32),
                *bufs(2, toks, dtype=F32),
                pltpu.VMEM((3, n_blocks * SLOTS, toks), BF16),
                pltpu.VMEM((3, n_blocks * SLOTS, 1), F32),
                pltpu.VMEM((3, top_k, toks), jnp.int32),
                pltpu.VMEM((top_k, toks), F32),
                pltpu.SemaphoreType.DMA((3, N_SEND)),
                pltpu.SemaphoreType.DMA((3, N_RECV)),
                pltpu.SemaphoreType.DMA((10,)),
            ],
            compiler_params=pltpu.CompilerParams(collective_id=0, has_side_effects=True, vmem_limit_bytes=VMEM_CAP),
            name="moe_layer",
        )(tokens.reshape(toks // SLOTS, SLOTS, d_model), expert_ids.T, dev_slot.T, exp_slot.T, gate_wts.T, w_gate, w_up, w_down)
        return summed

    def moe_layer(*args):
        return jax.shard_map(device_layer, mesh=mesh, in_specs=(row_spec,) * 5 + (weight_spec,) * 3, out_specs=row_spec, check_vma=False)(*args)

    return moe_layer
```

```python
import jax
import jax.numpy as jnp
from jax import lax
from jax.experimental import pallas as pl
from jax.experimental.pallas import tpu as pltpu
from jax.sharding import PartitionSpec as P

STRIDE = (32, 8, 2)
RING = 4
SLOTS = 16
STEPS = (2, 1, -1)
VMEM_CAP = 65930000
BF16 = jnp.bfloat16
F32 = jnp.float32


def rem4(v):
    return lax.rem(v, RING)


class Place:
    def __init__(self):
        self.me = lax.axis_index("expert")
        self.core = lax.rem(self.me, 2)
        self.k = [rem4(lax.div(self.me, s)) for s in STRIDE]

    def peer(self, axis, delta, core=None):
        there = rem4(self.k[axis] + delta + RING)
        dev = self.me + (there - self.k[axis]) * STRIDE[axis]
        return dev if core is None else dev + core - self.core

    def partner(self):
        return self.me + 1 - 2 * self.core

    def greet(self):
        sem = pltpu.get_barrier_semaphore()
        peers = [self.peer(ax, dl, c) for ax in range(3) for dl in STEPS for c in (0, 1)] + [self.partner()]
        self.n_peers = len(peers)
        for dev in peers:
            pl.semaphore_signal(sem, inc=1, device_id={"expert": dev}, device_id_type=pl.DeviceIdType.MESH)

    def meet(self):
        pl.semaphore_wait(pltpu.get_barrier_semaphore(), self.n_peers)


def remote(src, dst, send, recv, dev):
    return pltpu.make_async_remote_copy(
        src_ref=src, dst_ref=dst, send_sem=send, recv_sem=recv, device_id={"expert": dev}, device_id_type=pl.DeviceIdType.MESH
    )


class Exchange:
    def __init__(self, pc, c, block, land, send, recv, base):
        self.pc, self.c, self.block, self.land = pc, c, block, land
        self.send, self.recv, self.base = send, recv, base

    def own(self, j):
        return j * 8 + self.pc.k[self.c] * 2 + self.pc.core

    def far(self, j):
        return self.to_ring(j, 2)

    def near(self, j):
        pc = self.pc
        sems = self.send, self.recv.at[self.base + j]
        across = remote(self.block(j * 8 + pc.k[self.c] * 2 + 1 - pc.core), self.land.at[self.own(j)], *sems, pc.partner())
        return self.to_ring(j, 1) + self.to_ring(j, -1) + [across]

    def to_ring(self, j, dl):
        pc, c = self.pc, self.c
        there = rem4(pc.k[c] + dl + RING)
        sems = self.send, self.recv.at[self.base + j]
        return [
            remote(self.block(j * 8 + there * 2 + core), self.land.at[self.own(j)], *sems, pc.peer(c, dl, core)) for core in range(2)
        ]

    def sends(self, j):
        return self.far(j) + self.near(j)

    def wait_land(self, j):
        rows = self.land.at[pl.ds(j * 8, 7)]
        remote(rows, rows, self.send, self.recv.at[self.base + j], self.pc.partner()).wait_recv()

    def wait_sent(self):
        rows = self.land.at[pl.ds(0, 7 * RING)]
        remote(rows, rows, self.send, self.recv.at[self.base], self.pc.partner()).wait_send()


def slots_of(rows, ids):
    return [ids[n:n + 1, :] == rows for n in range(ids.shape[0])]


R_META, R_A, R_FAR, R_SIDES, R_ENDS, R_BACK, R_B, R_SUM, N_RECV = 0, 2, 4, 5, 9, 11, 15, 20, 24
R_C = 0
S_META, S_GATHER, S_C, S_BACK, S_B, S_SUM, N_SEND = 0, 2, 3, 4, 5, 6, 7


def layer_kernel(dims, tok, ids, devs, exps, gates, wg, wu, wd, out, t0, t1, t2, mm, s0, s1, s2, l0, l1, l2, x, hid, vg, vu, vd, c0, c1, c2,
                 m0, m1, m2, a0, a1, a2, f0, f1, f2, g0, g1, g2, hot, scale, raw, hot_gate, send, recv, shared, here):
    widths, starts = dims
    pc = Place()
    ts, ss, ls, cs, ms, sums = (t0, t1, t2), (s0, s1, s2), (l0, l1, l2), (c0, c1, c2), (m0, m1, m2), (a0, a1, a2)
    fars, nears = (f0, f1, f2), (g0, g1, g2)
    axes = [(p, (p + 1) % 3, (p + 2) % 3) for p in range(3)]
    back = [axes[(p + 2) % 3] for p in range(3)]
    k = pc.k
    toks = mm.shape[-1]
    top_k = ids.shape[0]
    half = toks // 2

    def spot(p, da, db):
        a, b, c = axes[p]
        return rem4(k[b] + db) * RING + rem4(k[a] + da)

    def blk(p, da, db):
        return ts[p].at[pl.ds(spot(p, da, db) * 8, 8)]

    def half_blk(p, da, db, d):
        return ts[p].at[pl.ds(spot(p, da, db) * 8 + d * 4, 4)]

    loads = [
        pltpu.make_async_copy(tok.at[:, :, pl.ds(starts[p], widths[p])], blk(p, 0, 0), here.at[p]) for p in range(3)
    ]
    routes = [pltpu.make_async_copy(src, raw.at[n], here.at[6 + n]) for n, src in enumerate((ids, devs, exps))]
    routes.append(pltpu.make_async_copy(gates, hot_gate, here.at[9]))
    weights = [pltpu.make_async_copy(src.at[0], dst, here.at[3 + n]) for n, (src, dst) in enumerate(((wg, vg), (wu, vu), (wd, vd)))]
    for cp in routes + loads:
        cp.start()
    with jax.named_scope("barrier"):
        pc.greet()
        for cp in routes:
            cp.wait()
        kept = (raw[1] >= 0) & (raw[2] >= 0)
        dest = jnp.where(kept, raw[0] * SLOTS + raw[1], -1).astype(F32)
        gate_bf = hot_gate[...].astype(BF16).astype(F32)
        for p, (a, b, c) in enumerate(axes):
            mm[p, k[b], k[a], pl.ds(0, top_k)] = dest
            mm[p, k[b], k[a], pl.ds(top_k, top_k)] = gate_bf
        for cp in loads:
            cp.wait()
        pc.meet()

    def push(p, s, r, ref, dev):
        remote(ref, ref, send.at[p, s], recv.at[p, r], dev).start()

    def got(p, r, ref):
        remote(ref, ref, send.at[p, 0], recv.at[p, r], pc.partner()).wait_recv()

    def gone(p, s, ref):
        remote(ref, ref, send.at[p, s], recv.at[p, 0], pc.partner()).wait_send()

    def some(p, n):
        return ts[p].at[pl.ds(0, n * 8)]

    def meta_of(p, da):
        return mm.at[p, k[axes[p][1]], rem4(k[axes[p][0]] + da + RING)]

    def along_b(p, da):
        for dl in (1, -1):
            push(p, S_GATHER, R_SIDES + da, blk(p, da, 0), pc.peer(axes[p][1], dl))

    def b_sides(p, da):
        got(p, R_SIDES + da, some(p, 2))
        dl = 1 if da in (0, 2) else -1
        push(p, S_GATHER, R_ENDS + (da in (1, 2)), blk(p, da, 3 if dl == 1 else 1), pc.peer(axes[p][1], dl))

    def b_ends(p, n):
        got(p, R_ENDS + n, some(p, 2))

    early = rem4(k[0] + k[1] + k[2] + 2)
    row = lax.broadcasted_iota(jnp.int32, (8 * SLOTS, toks), 0)

    def pick(p, da, db):
        a, b, c = axes[p]
        aa, bb = rem4(k[a] + da), rem4(k[b] + db)
        j = rem4(aa + bb + k[c])
        first = SLOTS * (pc.me - k[c] * STRIDE[c] - pc.core)
        rows = (first + (row >> 5) * (SLOTS * STRIDE[c]) + (row & 31)).astype(F32)
        ids = mm[p, bb, aa][:top_k]
        chosen = sum(jnp.where(hit, 1.0, 0.0) for hit in slots_of(rows, ids)).astype(BF16)
        block = ts[p][pl.ds((bb * RING + aa) * 8, 8)].reshape(toks, widths[p])
        picked = jnp.dot(chosen, block, preferred_element_type=F32).astype(BF16)
        ss[p][pl.ds(j * 8, 8), bb] = picked.reshape(8, SLOTS, widths[p])

    def sides(p, da):
        @pl.loop(0, 2)
        def _(q):
            pick(p, da, 3 - 2 * q)

    to_expert = [
        Exchange(pc, axes[p][2], (lambda n, p=p: ss[p].at[n]), ls[p], send.at[p, S_C], shared, R_C) for p in range(3)
    ]
    def offer(p, j, far=True, near=True):
        line = to_expert[p]
        for cp in (line.far(j) if far else []) + (line.near(j) if near else []):
            cp.start()
        if near:
            ls[p][line.own(j)] = ss[p][line.own(j)]

    for p in range(3):
        for dl in STEPS:
            push(p, S_META, R_META, meta_of(p, 0), pc.peer(axes[p][0], dl))
        push(p, S_GATHER, R_A, blk(p, 0, 0), pc.peer(axes[p][0], 1))
        push(p, S_GATHER, R_A + 1, blk(p, 0, 0), pc.peer(axes[p][0], -1))
    for p in range(3):
        along_b(p, 0)
    for cp in weights:
        cp.start()
    with jax.named_scope("ag_meta"):
        for p in range(3):
            got(p, R_META, mm.at[p, 0, pl.ds(0, 3)])
            for dl in STEPS:
                push(p, S_META + 1, R_META + 1, mm.at[p, k[axes[p][1]]], pc.peer(axes[p][1], dl))
    with jax.named_scope("ag_a"):
        for p in range(3):
            got(p, R_A, blk(p, 3, 0))
            push(p, S_GATHER, R_FAR, half_blk(p, 3, 0, 0), pc.peer(axes[p][0], 1))
            got(p, R_A + 1, blk(p, 1, 0))
            push(p, S_GATHER, R_FAR, half_blk(p, 1, 0, 1), pc.peer(axes[p][0], -1))
        for p in range(3):
            along_b(p, 3)
        for p in range(3):
            along_b(p, 1)
    with jax.named_scope("pick0"):
        for p in range(3):
            @pl.loop(0, 3)
            def _(q):
                pick(p, q + lax.div(q, 2), 0)
    with jax.named_scope("ag_a2"):
        for p in range(3):
            got(p, R_FAR, blk(p, 2, 0))
            along_b(p, 2)
    with jax.named_scope("ag_b0"):
        for p in range(3):
            b_sides(p, 0)
    for p in range(3):
        got(p, R_META + 1, mm.at[p, pl.ds(0, 3)])
    with jax.named_scope("pick1"):
        for p in range(3):
            pick(p, 2, 0)
            sides(p, 0)
    for da in (3, 1):
        with jax.named_scope("ag_b13"):
            for p in range(3):
                b_sides(p, da)
        with jax.named_scope("pick13"):
            for p in range(3):
                sides(p, da)
    with jax.named_scope("ag_b2"):
        for p in range(3):
            b_sides(p, 2)
    with jax.named_scope("pick2"):
        for p in range(3):
            sides(p, 2)
    to_source = [
        Exchange(pc, back[p][2], (lambda n, p=p: ts[p].at[pl.ds(n * RING, RING)]), cs[p], send.at[p, S_BACK], recv.at[p], R_BACK)
        for p in range(3)
    ]

    for p in (2, 1, 0):
        with jax.named_scope("ag_b3"):
            b_ends(p, 0)
        with jax.named_scope("pick3"):
            @pl.loop(0, 2)
            def _(q):
                pick(p, 3 * q, 2)

            offer(p, early, near=p > 0)
    for p in (2, 1, 0):
        with jax.named_scope("ag_b4"):
            b_ends(p, 1)
        with jax.named_scope("pick4"):
            @pl.loop(0, 2)
            def _(q):
                pick(p, 1 + q, 2)

            if p:
                @pl.loop(0, RING - 1)
                def _(q):
                    offer(p, q + lax.div(q + RING - early, RING))
            else:
                @pl.loop(0, RING)
                def _(j):
                    @pl.when(j != early)
                    def _():
                        offer(p, j, near=False)

                    offer(p, j, far=False)

    for cp in weights:
        cp.wait()
    for p in range(3):
        gone(p, S_META, mm.at[p, 0, pl.ds(0, 3)])
        gone(p, S_META + 1, mm.at[p, pl.ds(0, 3)])
        gone(p, S_GATHER, some(p, 15))

    def places(order, j, zy, core):
        z, yy = lax.div(zy, RING), rem4(zy)
        at = (z, yy, rem4(j + 2 * RING - z - yy))
        return [(j * 8 + at[c] * 2 + core, at[b]) for a, b, c in order]

    def ffn(j):
        @pl.loop(0, RING * RING)
        def _(zy):
            for core in range(2):
                for p, (at, bb) in enumerate(places(axes, j, zy, core)):
                    x[pl.ds(pl.multiple_of((zy * 2 + core) * SLOTS, SLOTS), SLOTS), pl.ds(starts[p], widths[p])] = ls[p][at, bb]

        g = jnp.dot(x[...], vg[...], preferred_element_type=F32)
        u = jnp.dot(x[...], vu[...], preferred_element_type=F32)
        hid[...] = (g * jax.nn.sigmoid(g) * u).astype(BF16)
        x[...] = jnp.dot(hid[...], vd[...], preferred_element_type=F32).astype(BF16)

        @pl.loop(0, RING * RING)
        def _(zy):
            for core in range(2):
                for p, (at, bb) in enumerate(places(back, j, zy, core)):
                    ts[p][at * RING + bb] = x[pl.ds(pl.multiple_of((zy * 2 + core) * SLOTS, SLOTS), SLOTS), pl.ds(starts[p], widths[p])]

    @pl.loop(0, RING)
    def _(j):
        with jax.named_scope("land"):
            full = x.at[pl.ds(0, 7 * RING * SLOTS)]
            remote(full, full, send.at[0, S_C], shared.at[R_C + j], pc.partner()).wait_recv()
        with jax.named_scope("ffn"):
            ffn(j)
        with jax.named_scope("send2"):
            for p, line in enumerate(to_source):
                for cp in line.sends(j):
                    cp.start()
                cs[p][line.own(j)] = ts[p][pl.ds(line.own(j) * RING, RING)]

    cut = 128 * ((widths[0] // 128 + 1) // 2)
    piece = [[pl.ds(0, cut), pl.ds(cut, w - cut)] for w in widths]

    def second(p, j):
        b = back[p][1]
        return [
            remote(cs[p].at[pl.ds(j * 8, 8), rem4(k[b] + dl + RING), :, piece[p][u]], ms[p].at[j * RING + k[b], :, :, piece[p][u]],
                   send.at[p, S_B], recv.at[p, R_B + j + u * lax.div(j, RING - 1)], pc.peer(b, dl))
            for u in range(2) for dl in STEPS
        ]

    @pl.loop(0, RING)
    def _(j):
        with jax.named_scope("land2"):
            for p, line in enumerate(to_source):
                line.wait_land(j)
                for cp in second(p, j):
                    cp.start()
        for p in range(3):
            kb = k[back[p][1]]
            ms[p][j * RING + kb] = cs[p][pl.ds(j * 8, 8), kb]

    def prepare(p, j):
        a, b, c = back[p]
        src = rem4(j + 2 * RING - k[c] - k[b])
        first = SLOTS * (pc.me - k[b] * STRIDE[b] - k[c] * STRIDE[c] - pc.core)
        info = mm[(p + 2) % 3, k[b], src]
        rows = first + (row >> 5) * (SLOTS * STRIDE[c]) + (row & 31)

        @pl.loop(0, RING)
        def _(bb):
            hits = slots_of((rows + bb * (SLOTS * STRIDE[b])).astype(F32), info[:top_k])
            chosen = sum(jnp.where(hit, 1.0, 0.0) for hit in hits)
            gate = sum(jnp.where(hit, info[top_k + n:top_k + n + 1, :], 0.0) for n, hit in enumerate(hits))
            at = pl.ds(pl.multiple_of(bb * 8 * SLOTS, 8 * SLOTS), 8 * SLOTS)
            hot[p, at] = chosen.astype(BF16)
            scale[at, p:p + 1] = jnp.sum(gate, axis=1, keepdims=True)

    def combine(p, j, cols):
        a, b, c = back[p]
        src = rem4(j + 2 * RING - k[c] - k[b])
        xcols = pl.ds(starts[p] + cols.start, cols.size)

        @pl.loop(0, RING)
        def _(bb):
            at = pl.ds(pl.multiple_of(bb * 8 * SLOTS, 8 * SLOTS), 8 * SLOTS)
            rows = ms[p][j * RING + bb, :, :, cols].reshape(8 * SLOTS, cols.size)
            x[at, xcols] = (rows.astype(F32) * scale[at, p:p + 1]).astype(BF16)

        sums[p][src, :, cols] = lax.dot_general(hot[p], x[:, xcols], (((0,), (0,)), ((), ())), preferred_element_type=F32)

    def prepared(j):
        with jax.named_scope("prepare"):
            for p in range(3):
                prepare(p, j)

    @pl.loop(0, RING - 1)
    def _(j):
        prepared(j)
        for p in range(3):
            with jax.named_scope("arrive"):
                got(p, R_B + j, ms[p].at[pl.ds(j * RING, 3)])
            with jax.named_scope("combine"):
                combine(p, j, pl.ds(0, widths[p]))

    prepared(RING - 1)

    def hand(p, r, ref, dst, dl):
        remote(ref, dst, send.at[p, S_SUM], recv.at[p, R_SUM + r], pc.peer(back[p][0], dl)).start()

    sides_of = ((0, 1), (1, -1))
    for u in range(2):
        for p in range(3):
            cols = piece[p][u]
            with jax.named_scope("arrive"):
                got(p, R_B + RING - 1 + u, ms[p].at[pl.ds((RING - 1) * RING, 3), :, :, cols])
            with jax.named_scope("combine"):
                combine(p, RING - 1, cols)
            ka = k[back[p][0]]
            for d, dl in sides_of:
                hand(p, u, sums[p].at[rem4(ka + 2), pl.ds(d * half, half), cols], fars[p].at[d, :, cols], dl)
            for d, dl in sides_of:
                rows = pl.ds((1 - d) * half, half)
                hand(p, 2 + u, sums[p].at[rem4(ka + dl + RING), rows, cols], nears[p].at[d, rows, cols], dl)
    for u in range(2):
        with jax.named_scope("rs1"):
            for p in range(3):
                cols = piece[p][u]
                ka = k[back[p][0]]
                got(p, R_SUM + u, fars[p].at[:, :, cols])
                for d, dl in sides_of:
                    near = rem4(ka + dl + RING)
                    rows = pl.ds(d * half, half)
                    sums[p][near, rows, cols] = sums[p][near, rows, cols] + fars[p][d, :, cols]
                    hand(p, 2 + u, sums[p].at[near, rows, cols], nears[p].at[d, rows, cols], dl)
    for u in range(2):
        with jax.named_scope("rs2"):
            for p in range(3):
                cols = piece[p][u]
                got(p, R_SUM + 2 + u, nears[p].at[:, :, cols])
                total = sums[p][k[back[p][0]], :, cols] + nears[p][0, :, cols] + nears[p][1, :, cols]
                out[:, pl.ds(starts[p] + cols.start, cols.size)] = total.astype(out.dtype)
    with jax.named_scope("drain"):
        for p in range(3):
            to_expert[p].wait_sent()
            to_source[p].wait_sent()
            gone(p, S_B, ms[p].at[pl.ds(0, 3 * RING)])
            gone(p, S_SUM, sums[p].at[pl.ds(0, 3)])


def solution(mesh):
    row_spec = P(("data", "expert"), None)
    weight_spec = P("expert", None, None)
    any_spec = pl.BlockSpec(memory_space=pl.ANY)

    def device_layer(tokens, expert_ids, gate_wts, dev_slot, exp_slot, w_gate, w_up, w_down):
        toks, top_k = expert_ids.shape
        d_model, d_ff = w_gate.shape[1:]
        tiles = d_model // 128
        widths = [128 * (tiles - 2 * (tiles // 3)), 128 * (tiles // 3), 128 * (tiles // 3)]
        starts = [0, widths[0], widths[0] + widths[1]]
        dims = (widths, starts)
        n_blocks = 2 * RING * RING

        def bufs(*lead, dtype=BF16):
            return [pltpu.VMEM((*lead, w), dtype) for w in widths]

        summed = pl.pallas_call(
            lambda *refs: layer_kernel(dims, *refs),
            out_shape=pltpu.VMEM((toks, d_model), BF16),
            in_specs=[any_spec] * 8,
            out_specs=pl.BlockSpec(memory_space=pltpu.VMEM),
            scratch_shapes=[
                *bufs(n_blocks * RING, SLOTS),
                pltpu.VMEM((3, RING, RING, 2 * top_k, toks), F32),
                *bufs(n_blocks, RING, SLOTS),
                *bufs(n_blocks, RING, SLOTS),
                pltpu.VMEM((n_blocks * SLOTS, d_model), BF16),
                pltpu.VMEM((n_blocks * SLOTS, d_ff), BF16),
                pltpu.VMEM((d_model, d_ff), BF16),
                pltpu.VMEM((d_model, d_ff), BF16),
                pltpu.VMEM((d_ff, d_model), BF16),
                *bufs(n_blocks, RING, SLOTS),
                *bufs(RING * RING, 8, SLOTS),
                *bufs(RING, toks, dtype=F32),
                *bufs(2, toks // 2, dtype=F32),
                *bufs(2, toks, dtype=F32),
                pltpu.VMEM((3, n_blocks * SLOTS, toks), BF16),
                pltpu.VMEM((n_blocks * SLOTS, 3), F32),
                pltpu.VMEM((3, top_k, toks), jnp.int32),
                pltpu.VMEM((top_k, toks), F32),
                pltpu.SemaphoreType.DMA((3, N_SEND)),
                pltpu.SemaphoreType.DMA((3, N_RECV)),
                pltpu.SemaphoreType.DMA((RING,)),
                pltpu.SemaphoreType.DMA((10,)),
            ],
            compiler_params=pltpu.CompilerParams(collective_id=0, has_side_effects=True, vmem_limit_bytes=VMEM_CAP),
            name="moe_layer",
        )(tokens.reshape(toks // SLOTS, SLOTS, d_model), expert_ids.T, dev_slot.T, exp_slot.T, gate_wts.T, w_gate, w_up, w_down)
        return summed

    def moe_layer(*args):
        return jax.shard_map(device_layer, mesh=mesh, in_specs=(row_spec,) * 5 + (weight_spec,) * 3, out_specs=row_spec, check_vma=False)(*args)

    return moe_layer
```

```python
import jax
import jax.numpy as jnp
from jax import lax
from jax.experimental import pallas as pl
from jax.experimental.pallas import tpu as pltpu
from jax.sharding import PartitionSpec as P

STRIDE = (32, 8, 2)
RING = 4
SLOTS = 16
STEPS = (2, 1, -1)
VMEM_CAP = 66400000
BF16 = jnp.bfloat16
F32 = jnp.float32


def rem4(v):
    return lax.rem(v, RING)


class Place:
    def __init__(self):
        self.me = lax.axis_index("expert")
        self.core = lax.rem(self.me, 2)
        self.grid = [rem4(lax.div(self.me, s)) for s in STRIDE]
        self.k, self.stride = self.turned(self.grid), self.turned(STRIDE)

    def turned(self, of):
        return [of[i] + self.core * (of[(i + 1) % 3] - of[i]) for i in range(3)]

    def peer(self, axis, delta, core=None):
        there = rem4(self.k[axis] + delta + RING)
        dev = self.me + (there - self.k[axis]) * self.stride[axis]
        return dev if core is None else dev + core - self.core

    def partner(self):
        return self.me + 1 - 2 * self.core

    def greet(self):
        sem = pltpu.get_barrier_semaphore()
        peers = [self.peer(ax, dl, c) for ax in range(3) for dl in STEPS for c in (0, 1)] + [self.partner()]
        self.n_peers = len(peers)
        for dev in peers:
            pl.semaphore_signal(sem, inc=1, device_id={"expert": dev}, device_id_type=pl.DeviceIdType.MESH)

    def meet(self):
        pl.semaphore_wait(pltpu.get_barrier_semaphore(), self.n_peers)


def remote(src, dst, send, recv, dev):
    return pltpu.make_async_remote_copy(
        src_ref=src, dst_ref=dst, send_sem=send, recv_sem=recv, device_id={"expert": dev}, device_id_type=pl.DeviceIdType.MESH
    )


class Exchange:
    def __init__(self, pc, c, block, land, send, recv, base, by_target=False):
        self.pc, self.c, self.block, self.land = pc, c, block, land
        self.send, self.recv, self.base = send, recv, base
        ours = pc.k[c], pc.stride[c]
        if by_target:
            turn = [(c + core) % 3 for core in range(2)]
            self.ring = [(pc.grid[ax], STRIDE[ax]) for ax in turn]
            self.beside = pc.grid[turn[1]] + pc.core * (pc.grid[turn[0]] - pc.grid[turn[1]])
        else:
            self.ring = [ours, ours]
            self.beside = pc.k[c]

    def slot(self, j, at):
        return j * 8 + at * 2 + self.pc.core

    def own(self, j):
        return self.slot(j, self.pc.k[self.c])

    def far(self, j):
        return self.to_ring(j, 2)

    def near(self, j):
        pc = self.pc
        sems = self.send, self.recv.at[self.base + j]
        across = remote(self.block(j * 8 + self.beside * 2 + 1 - pc.core), self.land.at[self.slot(j, self.beside)], *sems, pc.partner())
        return self.to_ring(j, 1) + self.to_ring(j, -1) + [across]

    def to_ring(self, j, dl):
        pc = self.pc
        sems = self.send, self.recv.at[self.base + j]
        out = []
        for core, (at, stride) in enumerate(self.ring):
            there = rem4(at + dl + RING)
            dev = pc.me + (there - at) * stride + core - pc.core
            out.append(remote(self.block(j * 8 + there * 2 + core), self.land.at[self.slot(j, at)], *sems, dev))
        return out

    def sends(self, j):
        return self.far(j) + self.near(j)

    def wait_land(self, j):
        rows = self.land.at[pl.ds(j * 8, 7)]
        remote(rows, rows, self.send, self.recv.at[self.base + j], self.pc.partner()).wait_recv()

    def wait_sent(self):
        rows = self.land.at[pl.ds(0, 7 * RING)]
        remote(rows, rows, self.send, self.recv.at[self.base], self.pc.partner()).wait_send()


def slots_of(rows, ids):
    return [ids[n:n + 1, :] == rows for n in range(ids.shape[0])]


R_META, R_A, R_FAR, R_SIDES, R_ENDS, R_BACK, R_B, R_SUM, N_RECV = 0, 2, 4, 5, 9, 11, 15, 20, 24
R_C = 0
S_META, S_GATHER, S_C, S_BACK, S_B, S_SUM, N_SEND = 0, 2, 3, 4, 5, 6, 7


def layer_kernel(dims, tok, ids, devs, exps, gates, wg, wu, wd, out, t0, t1, t2, mm, s0, s1, s2, l0, l1, l2, x, hid, vg, vu, vd, c0, c1, c2,
                 m0, m1, m2, a0, a1, a2, f0, f1, f2, g0, g1, g2, hot, scale, raw, hot_gate, send, recv, shared, here):
    widths, starts = dims
    pc = Place()
    ts, ss, ls, cs, ms, sums = (t0, t1, t2), (s0, s1, s2), (l0, l1, l2), (c0, c1, c2), (m0, m1, m2), (a0, a1, a2)
    fars, nears = (f0, f1, f2), (g0, g1, g2)
    axes = [(p, (p + 1) % 3, (p + 2) % 3) for p in range(3)]
    back = [axes[(p + 2) % 3] for p in range(3)]
    k = pc.k
    toks = mm.shape[-1]
    top_k = ids.shape[0]
    half = toks // 2

    def spot(p, da, db):
        a, b, c = axes[p]
        return rem4(k[b] + db) * RING + rem4(k[a] + da)

    def blk(p, da, db):
        return ts[p].at[pl.ds(spot(p, da, db) * 8, 8)]

    def half_blk(p, da, db, d):
        return ts[p].at[pl.ds(spot(p, da, db) * 8 + d * 4, 4)]

    loads = [
        pltpu.make_async_copy(tok.at[:, :, pl.ds(starts[p], widths[p])], blk(p, 0, 0), here.at[p]) for p in range(3)
    ]
    routes = [pltpu.make_async_copy(src, raw.at[n], here.at[6 + n]) for n, src in enumerate((ids, devs, exps))]
    routes.append(pltpu.make_async_copy(gates, hot_gate, here.at[9]))
    weights = [pltpu.make_async_copy(src.at[0], dst, here.at[3 + n]) for n, (src, dst) in enumerate(((wg, vg), (wu, vu), (wd, vd)))]
    for cp in routes + loads:
        cp.start()
    with jax.named_scope("barrier"):
        pc.greet()
        for cp in routes:
            cp.wait()
        kept = (raw[1] >= 0) & (raw[2] >= 0)
        dest = jnp.where(kept, raw[0] * SLOTS + raw[1], -1).astype(F32)
        gate_bf = hot_gate[...].astype(BF16).astype(F32)
        for p, (a, b, c) in enumerate(axes):
            mm[p, k[b], k[a], pl.ds(0, top_k)] = dest
            mm[p, k[b], k[a], pl.ds(top_k, top_k)] = gate_bf
        for cp in loads:
            cp.wait()
        pc.meet()

    def push(p, s, r, ref, dev):
        remote(ref, ref, send.at[p, s], recv.at[p, r], dev).start()

    def got(p, r, ref):
        remote(ref, ref, send.at[p, 0], recv.at[p, r], pc.partner()).wait_recv()

    def gone(p, s, ref):
        remote(ref, ref, send.at[p, s], recv.at[p, 0], pc.partner()).wait_send()

    def some(p, n):
        return ts[p].at[pl.ds(0, n * 8)]

    def meta_of(p, da):
        return mm.at[p, k[axes[p][1]], rem4(k[axes[p][0]] + da + RING)]

    def along_b(p, da):
        for dl in (1, -1):
            push(p, S_GATHER, R_SIDES + da, blk(p, da, 0), pc.peer(axes[p][1], dl))

    def b_sides(p, da):
        got(p, R_SIDES + da, some(p, 2))
        dl = 1 if da in (0, 2) else -1
        push(p, S_GATHER, R_ENDS + (da in (1, 2)), blk(p, da, 3 if dl == 1 else 1), pc.peer(axes[p][1], dl))

    def b_ends(p, n):
        got(p, R_ENDS + n, some(p, 2))

    early = rem4(k[0] + k[1] + k[2] + 2)
    row = lax.broadcasted_iota(jnp.int32, (8 * SLOTS, toks), 0)

    def pick(p, da, db):
        a, b, c = axes[p]
        aa, bb = rem4(k[a] + da), rem4(k[b] + db)
        j = rem4(aa + bb + k[c])
        first = SLOTS * (pc.me - k[c] * pc.stride[c] - pc.core)
        rows = (first + (row >> 5) * (SLOTS * pc.stride[c]) + (row & 31)).astype(F32)
        ids = mm[p, bb, aa][:top_k]
        chosen = sum(jnp.where(hit, 1.0, 0.0) for hit in slots_of(rows, ids)).astype(BF16)
        block = ts[p][pl.ds((bb * RING + aa) * 8, 8)].reshape(toks, widths[p])
        picked = jnp.dot(chosen, block, preferred_element_type=F32).astype(BF16)
        ss[p][pl.ds(j * 8, 8), bb] = picked.reshape(8, SLOTS, widths[p])

    def sides(p, da):
        @pl.loop(0, 2)
        def _(q):
            pick(p, da, 3 - 2 * q)

    to_expert = [
        Exchange(pc, axes[p][2], (lambda n, p=p: ss[p].at[n]), ls[p], send.at[p, S_C], shared, R_C) for p in range(3)
    ]
    def offer(p, j, far=True, near=True):
        line = to_expert[p]
        for cp in (line.far(j) if far else []) + (line.near(j) if near else []):
            cp.start()
        if near:
            ls[p][line.own(j)] = ss[p][line.own(j)]

    for p in range(3):
        for dl in STEPS:
            push(p, S_META, R_META, meta_of(p, 0), pc.peer(axes[p][0], dl))
        push(p, S_GATHER, R_A, blk(p, 0, 0), pc.peer(axes[p][0], 1))
        push(p, S_GATHER, R_A + 1, blk(p, 0, 0), pc.peer(axes[p][0], -1))
    for p in range(3):
        along_b(p, 0)
    for cp in weights:
        cp.start()
    with jax.named_scope("ag_meta"):
        for p in range(3):
            got(p, R_META, mm.at[p, 0, pl.ds(0, 3)])
            for dl in STEPS:
                push(p, S_META + 1, R_META + 1, mm.at[p, k[axes[p][1]]], pc.peer(axes[p][1], dl))
    with jax.named_scope("ag_a"):
        for p in range(3):
            got(p, R_A, blk(p, 3, 0))
            push(p, S_GATHER, R_FAR, half_blk(p, 3, 0, 0), pc.peer(axes[p][0], 1))
            got(p, R_A + 1, blk(p, 1, 0))
            push(p, S_GATHER, R_FAR, half_blk(p, 1, 0, 1), pc.peer(axes[p][0], -1))
        for p in range(3):
            along_b(p, 3)
        for p in range(3):
            along_b(p, 1)
    with jax.named_scope("pick0"):
        for p in range(3):
            @pl.loop(0, 3)
            def _(q):
                pick(p, q + lax.div(q, 2), 0)
    with jax.named_scope("ag_a2"):
        for p in range(3):
            got(p, R_FAR, blk(p, 2, 0))
            along_b(p, 2)
    with jax.named_scope("ag_b0"):
        for p in range(3):
            b_sides(p, 0)
    for p in range(3):
        got(p, R_META + 1, mm.at[p, pl.ds(0, 3)])
    with jax.named_scope("pick1"):
        for p in range(3):
            pick(p, 2, 0)
            sides(p, 0)
    for da in (3, 1):
        with jax.named_scope("ag_b13"):
            for p in range(3):
                b_sides(p, da)
        with jax.named_scope("pick13"):
            for p in range(3):
                sides(p, da)
    with jax.named_scope("ag_b2"):
        for p in range(3):
            b_sides(p, 2)
    with jax.named_scope("pick2"):
        for p in range(3):
            sides(p, 2)
    to_source = [
        Exchange(pc, back[p][2], (lambda n, p=p: ts[p].at[pl.ds(n * RING, RING)]), cs[p], send.at[p, S_BACK], recv.at[p], R_BACK, True)
        for p in range(3)
    ]

    for p in (2, 1, 0):
        with jax.named_scope("ag_b3"):
            b_ends(p, 0)
        with jax.named_scope("pick3"):
            @pl.loop(0, 2)
            def _(q):
                pick(p, 3 * q, 2)

            offer(p, early, near=p > 0)
    for p in (2, 1, 0):
        with jax.named_scope("ag_b4"):
            b_ends(p, 1)
        with jax.named_scope("pick4"):
            @pl.loop(0, 2)
            def _(q):
                pick(p, 1 + q, 2)

            if p:
                @pl.loop(0, RING - 1)
                def _(q):
                    offer(p, q + lax.div(q + RING - early, RING))
            else:
                @pl.loop(0, RING)
                def _(j):
                    @pl.when(j != early)
                    def _():
                        offer(p, j, near=False)

                    offer(p, j, far=False)

    def prepare(p, j, bank):
        a, b, c = back[p]
        src = rem4(j + 2 * RING - k[c] - k[b])
        first = SLOTS * (pc.me - k[b] * pc.stride[b] - k[c] * pc.stride[c] - pc.core)
        info = mm[(p + 2) % 3, k[b], src]
        rows = first + (row >> 5) * (SLOTS * pc.stride[c]) + (row & 31)

        @pl.loop(0, RING)
        def _(bb):
            hits = slots_of((rows + bb * (SLOTS * pc.stride[b])).astype(F32), info[:top_k])
            chosen = sum(jnp.where(hit, 1.0, 0.0) for hit in hits)
            gate = sum(jnp.where(hit, info[top_k + n:top_k + n + 1, :], 0.0) for n, hit in enumerate(hits))
            at = pl.ds(pl.multiple_of(bb * 8 * SLOTS, 8 * SLOTS), 8 * SLOTS)
            hot[bank, p, at] = chosen.astype(BF16)
            scale[at, 3 * bank + p:3 * bank + p + 1] = jnp.sum(gate, axis=1, keepdims=True)

    def prepared(j, bank):
        with jax.named_scope("prepare"):
            for p in range(3):
                prepare(p, j, bank)

    prepared(RING - 1, 1)
    prepared(0, 0)

    for cp in weights:
        cp.wait()
    for p in range(3):
        gone(p, S_META, mm.at[p, 0, pl.ds(0, 3)])
        gone(p, S_META + 1, mm.at[p, pl.ds(0, 3)])
        gone(p, S_GATHER, some(p, 15))

    def places(order, j, zy, core):
        z, yy = lax.div(zy, RING), rem4(zy)
        at = (z, yy, rem4(j + 2 * RING - z - yy))
        return [(j * 8 + at[(c + core) % 3] * 2 + core, at[(b + core) % 3]) for a, b, c in order]

    def ffn(j):
        @pl.loop(0, RING * RING)
        def _(zy):
            for core in range(2):
                for p, (at, bb) in enumerate(places(axes, j, zy, core)):
                    x[pl.ds(pl.multiple_of((zy * 2 + core) * SLOTS, SLOTS), SLOTS), pl.ds(starts[p], widths[p])] = ls[p][at, bb]

        g = jnp.dot(x[...], vg[...], preferred_element_type=F32)
        u = jnp.dot(x[...], vu[...], preferred_element_type=F32)
        hid[...] = (g * jax.nn.sigmoid(g) * u).astype(BF16)
        x[...] = jnp.dot(hid[...], vd[...], preferred_element_type=F32).astype(BF16)

        @pl.loop(0, RING * RING)
        def _(zy):
            for core in range(2):
                for p, (at, bb) in enumerate(places(back, j, zy, core)):
                    ts[p][at * RING + bb] = x[pl.ds(pl.multiple_of((zy * 2 + core) * SLOTS, SLOTS), SLOTS), pl.ds(starts[p], widths[p])]

    @pl.loop(0, RING)
    def _(j):
        with jax.named_scope("land"):
            full = x.at[pl.ds(0, 7 * RING * SLOTS)]
            remote(full, full, send.at[0, S_C], shared.at[R_C + j], pc.partner()).wait_recv()
        with jax.named_scope("ffn"):
            ffn(j)
        with jax.named_scope("send2"):
            for p, line in enumerate(to_source):
                for cp in line.sends(j):
                    cp.start()
                cs[p][line.own(j)] = ts[p][pl.ds(line.own(j) * RING, RING)]

    cut = 128 * ((widths[0] // 128 + 1) // 2)
    piece = [[pl.ds(0, cut), pl.ds(cut, w - cut)] for w in widths]

    def second(p, j):
        b = back[p][1]
        return [
            remote(cs[p].at[pl.ds(j * 8, 8), rem4(k[b] + dl + RING), :, piece[p][u]], ms[p].at[j * RING + k[b], :, :, piece[p][u]],
                   send.at[p, S_B], recv.at[p, R_B + j + u * lax.div(j, RING - 1)], pc.peer(b, dl))
            for u in range(2) for dl in STEPS
        ]

    @pl.loop(0, RING)
    def _(j):
        with jax.named_scope("land2"):
            for p, line in enumerate(to_source):
                line.wait_land(j)
                for cp in second(p, j):
                    cp.start()
        for p in range(3):
            kb = k[back[p][1]]
            ms[p][j * RING + kb] = cs[p][pl.ds(j * 8, 8), kb]

    def combine(p, j, cols, bank):
        a, b, c = back[p]
        src = rem4(j + 2 * RING - k[c] - k[b])
        xcols = pl.ds(starts[p] + cols.start, cols.size)

        @pl.loop(0, RING)
        def _(bb):
            at = pl.ds(pl.multiple_of(bb * 8 * SLOTS, 8 * SLOTS), 8 * SLOTS)
            rows = ms[p][j * RING + bb, :, :, cols].reshape(8 * SLOTS, cols.size)
            x[at, xcols] = (rows.astype(F32) * scale[at, 3 * bank + p:3 * bank + p + 1]).astype(BF16)

        sums[p][src, :, cols] = lax.dot_general(hot[bank, p], x[:, xcols], (((0,), (0,)), ((), ())), preferred_element_type=F32)

    @pl.loop(0, RING - 1)
    def _(j):
        for p in range(3):
            with jax.named_scope("arrive"):
                got(p, R_B + j, ms[p].at[pl.ds(j * RING, 3)])
            with jax.named_scope("combine"):
                combine(p, j, pl.ds(0, widths[p]), 0)

        @pl.when(j < RING - 2)
        def _():
            prepared(j + 1, 0)


    def hand(p, r, ref, dst, dl):
        remote(ref, dst, send.at[p, S_SUM], recv.at[p, R_SUM + r], pc.peer(back[p][0], dl)).start()

    sides_of = ((0, 1), (1, -1))
    for u in range(2):
        for p in range(3):
            cols = piece[p][u]
            with jax.named_scope("arrive"):
                got(p, R_B + RING - 1 + u, ms[p].at[pl.ds((RING - 1) * RING, 3), :, :, cols])
            with jax.named_scope("combine"):
                combine(p, RING - 1, cols, 1)
            ka = k[back[p][0]]
            for d, dl in sides_of:
                hand(p, u, sums[p].at[rem4(ka + 2), pl.ds(d * half, half), cols], fars[p].at[d, :, cols], dl)
            for d, dl in sides_of:
                rows = pl.ds((1 - d) * half, half)
                hand(p, 2 + u, sums[p].at[rem4(ka + dl + RING), rows, cols], nears[p].at[d, rows, cols], dl)
    for u in range(2):
        with jax.named_scope("rs1"):
            for p in range(3):
                cols = piece[p][u]
                ka = k[back[p][0]]
                got(p, R_SUM + u, fars[p].at[:, :, cols])
                for d, dl in sides_of:
                    near = rem4(ka + dl + RING)
                    rows = pl.ds(d * half, half)
                    sums[p][near, rows, cols] = sums[p][near, rows, cols] + fars[p][d, :, cols]
                    hand(p, 2 + u, sums[p].at[near, rows, cols], nears[p].at[d, rows, cols], dl)
    for u in range(2):
        with jax.named_scope("rs2"):
            for p in range(3):
                cols = piece[p][u]
                got(p, R_SUM + 2 + u, nears[p].at[:, :, cols])
                total = sums[p][k[back[p][0]], :, cols] + nears[p][0, :, cols] + nears[p][1, :, cols]
                out[:, pl.ds(starts[p] + cols.start, cols.size)] = total.astype(out.dtype)
    with jax.named_scope("drain"):
        for p in range(3):
            to_expert[p].wait_sent()
            to_source[p].wait_sent()
            gone(p, S_B, ms[p].at[pl.ds(0, 3 * RING)])
            gone(p, S_SUM, sums[p].at[pl.ds(0, 3)])


def solution(mesh):
    row_spec = P(("data", "expert"), None)
    weight_spec = P("expert", None, None)
    any_spec = pl.BlockSpec(memory_space=pl.ANY)

    def device_layer(tokens, expert_ids, gate_wts, dev_slot, exp_slot, w_gate, w_up, w_down):
        toks, top_k = expert_ids.shape
        d_model, d_ff = w_gate.shape[1:]
        tiles = d_model // 128
        widths = [128 * (tiles - 2 * (tiles // 3)), 128 * (tiles // 3), 128 * (tiles // 3)]
        starts = [0, widths[0], widths[0] + widths[1]]
        dims = (widths, starts)
        n_blocks = 2 * RING * RING

        def bufs(*lead, dtype=BF16):
            return [pltpu.VMEM((*lead, w), dtype) for w in widths]

        summed = pl.pallas_call(
            lambda *refs: layer_kernel(dims, *refs),
            out_shape=pltpu.VMEM((toks, d_model), BF16),
            in_specs=[any_spec] * 8,
            out_specs=pl.BlockSpec(memory_space=pltpu.VMEM),
            scratch_shapes=[
                *bufs(n_blocks * RING, SLOTS),
                pltpu.VMEM((3, RING, RING, 2 * top_k, toks), F32),
                *bufs(n_blocks, RING, SLOTS),
                *bufs(n_blocks, RING, SLOTS),
                pltpu.VMEM((n_blocks * SLOTS, d_model), BF16),
                pltpu.VMEM((n_blocks * SLOTS, d_ff), BF16),
                pltpu.VMEM((d_model, d_ff), BF16),
                pltpu.VMEM((d_model, d_ff), BF16),
                pltpu.VMEM((d_ff, d_model), BF16),
                *bufs(n_blocks, RING, SLOTS),
                *bufs(RING * RING, 8, SLOTS),
                *bufs(RING, toks, dtype=F32),
                *bufs(2, toks // 2, dtype=F32),
                *bufs(2, toks, dtype=F32),
                pltpu.VMEM((2, 3, n_blocks * SLOTS, toks), BF16),
                pltpu.VMEM((n_blocks * SLOTS, 6), F32),
                pltpu.VMEM((3, top_k, toks), jnp.int32),
                pltpu.VMEM((top_k, toks), F32),
                pltpu.SemaphoreType.DMA((3, N_SEND)),
                pltpu.SemaphoreType.DMA((3, N_RECV)),
                pltpu.SemaphoreType.DMA((RING,)),
                pltpu.SemaphoreType.DMA((10,)),
            ],
            compiler_params=pltpu.CompilerParams(collective_id=0, has_side_effects=True, vmem_limit_bytes=VMEM_CAP),
            name="moe_layer",
        )(tokens.reshape(toks // SLOTS, SLOTS, d_model), expert_ids.T, dev_slot.T, exp_slot.T, gate_wts.T, w_gate, w_up, w_down)
        return summed

    def moe_layer(*args):
        return jax.shard_map(device_layer, mesh=mesh, in_specs=(row_spec,) * 5 + (weight_spec,) * 3, out_specs=row_spec, check_vma=False)(*args)

    return moe_layer
```

```python
import jax
import jax.numpy as jnp
from jax import lax
from jax.experimental import pallas as pl
from jax.experimental.pallas import tpu as pltpu
from jax.sharding import PartitionSpec as P

STRIDE = (32, 8, 2)
RING = 4
SLOTS = 16
STEPS = (2, 1, -1)
VMEM_CAP = 66400000
BF16 = jnp.bfloat16
F32 = jnp.float32


def rem4(v):
    return lax.rem(v, RING)


class Place:
    def __init__(self):
        self.me = lax.axis_index("expert")
        self.core = lax.rem(self.me, 2)
        self.grid = [rem4(lax.div(self.me, s)) for s in STRIDE]
        self.k, self.stride = self.turned(self.grid), self.turned(STRIDE)

    def turned(self, of):
        return [of[i] + self.core * (of[(i + 1) % 3] - of[i]) for i in range(3)]

    def peer(self, axis, delta, core=None):
        there = rem4(self.k[axis] + delta + RING)
        dev = self.me + (there - self.k[axis]) * self.stride[axis]
        return dev if core is None else dev + core - self.core

    def partner(self):
        return self.me + 1 - 2 * self.core

    def greet(self):
        sem = pltpu.get_barrier_semaphore()
        peers = [self.peer(ax, dl, c) for ax in range(3) for dl in STEPS for c in (0, 1)] + [self.partner()]
        self.n_peers = len(peers)
        for dev in peers:
            pl.semaphore_signal(sem, inc=1, device_id={"expert": dev}, device_id_type=pl.DeviceIdType.MESH)

    def meet(self):
        pl.semaphore_wait(pltpu.get_barrier_semaphore(), self.n_peers)


def remote(src, dst, send, recv, dev):
    return pltpu.make_async_remote_copy(
        src_ref=src, dst_ref=dst, send_sem=send, recv_sem=recv, device_id={"expert": dev}, device_id_type=pl.DeviceIdType.MESH
    )


class Exchange:
    def __init__(self, pc, c, block, land, send, recv, base, by_target=False):
        self.pc, self.c, self.block, self.land = pc, c, block, land
        self.send, self.recv, self.base = send, recv, base
        ours = pc.k[c], pc.stride[c]
        if by_target:
            turn = [(c + core) % 3 for core in range(2)]
            self.ring = [(pc.grid[ax], STRIDE[ax]) for ax in turn]
            self.beside = pc.grid[turn[1]] + pc.core * (pc.grid[turn[0]] - pc.grid[turn[1]])
        else:
            self.ring = [ours, ours]
            self.beside = pc.k[c]

    def slot(self, j, at):
        return j * 8 + at * 2 + self.pc.core

    def own(self, j):
        return self.slot(j, self.pc.k[self.c])

    def far(self, j):
        return self.to_ring(j, 2)

    def near(self, j):
        pc = self.pc
        sems = self.send, self.recv.at[self.base + j]
        across = remote(self.block(j * 8 + self.beside * 2 + 1 - pc.core), self.land.at[self.slot(j, self.beside)], *sems, pc.partner())
        return self.to_ring(j, 1) + self.to_ring(j, -1) + [across]

    def to_ring(self, j, dl):
        pc = self.pc
        sems = self.send, self.recv.at[self.base + j]
        out = []
        for core, (at, stride) in enumerate(self.ring):
            there = rem4(at + dl + RING)
            dev = pc.me + (there - at) * stride + core - pc.core
            out.append(remote(self.block(j * 8 + there * 2 + core), self.land.at[self.slot(j, at)], *sems, dev))
        return out

    def sends(self, j):
        return self.far(j) + self.near(j)

    def wait_land(self, j):
        rows = self.land.at[pl.ds(j * 8, 7)]
        remote(rows, rows, self.send, self.recv.at[self.base + j], self.pc.partner()).wait_recv()

    def wait_sent(self):
        rows = self.land.at[pl.ds(0, 7 * RING)]
        remote(rows, rows, self.send, self.recv.at[self.base], self.pc.partner()).wait_send()


def slots_of(rows, ids):
    return [ids[n:n + 1, :] == rows for n in range(ids.shape[0])]


R_META, R_A, R_FAR, R_SIDES, R_ENDS, R_BACK, R_B, R_SUM, N_RECV = 0, 2, 4, 5, 9, 11, 15, 20, 24
R_C = 0
S_META, S_GATHER, S_C, S_BACK, S_B, S_SUM, N_SEND = 0, 2, 3, 4, 5, 6, 7


def layer_kernel(dims, tok, ids, devs, exps, gates, wg, wu, wd, out, t0, t1, t2, mm, s0, s1, s2, l0, l1, l2, x, hid, vg, vu, vd, c0, c1, c2,
                 m0, m1, m2, a0, a1, a2, f0, f1, f2, g0, g1, g2, hot, scale, raw, hot_gate, send, recv, shared, here):
    widths, starts = dims
    pc = Place()
    ts, ss, ls, cs, ms, sums = (t0, t1, t2), (s0, s1, s2), (l0, l1, l2), (c0, c1, c2), (m0, m1, m2), (a0, a1, a2)
    fars, nears = (f0, f1, f2), (g0, g1, g2)
    axes = [(p, (p + 1) % 3, (p + 2) % 3) for p in range(3)]
    back = [axes[(p + 2) % 3] for p in range(3)]
    k = pc.k
    toks = mm.shape[-1]
    top_k = ids.shape[0]
    half = toks // 2

    def spot(p, da, db):
        a, b, c = axes[p]
        return rem4(k[b] + db) * RING + rem4(k[a] + da)

    def blk(p, da, db):
        return ts[p].at[pl.ds(spot(p, da, db) * 8, 8)]

    def half_blk(p, da, db, d):
        return ts[p].at[pl.ds(spot(p, da, db) * 8 + d * 4, 4)]

    loads = [
        pltpu.make_async_copy(tok.at[:, :, pl.ds(starts[p], widths[p])], blk(p, 0, 0), here.at[p]) for p in range(3)
    ]
    routes = [pltpu.make_async_copy(src, raw.at[n], here.at[6 + n]) for n, src in enumerate((ids, devs, exps))]
    routes.append(pltpu.make_async_copy(gates, hot_gate, here.at[9]))
    weights = [pltpu.make_async_copy(src.at[0], dst, here.at[3 + n]) for n, (src, dst) in enumerate(((wg, vg), (wu, vu), (wd, vd)))]
    for cp in routes + loads:
        cp.start()
    with jax.named_scope("barrier"):
        pc.greet()
        for cp in routes:
            cp.wait()
        kept = (raw[1] >= 0) & (raw[2] >= 0)
        dest = jnp.where(kept, raw[0] * SLOTS + raw[1], -1).astype(F32)
        gate_bf = hot_gate[...].astype(BF16).astype(F32)
        for p, (a, b, c) in enumerate(axes):
            mm[p, k[b], k[a], pl.ds(0, top_k)] = dest
            mm[p, k[b], k[a], pl.ds(top_k, top_k)] = gate_bf
        for cp in loads:
            cp.wait()
        pc.meet()

    def push(p, s, r, ref, dev):
        remote(ref, ref, send.at[p, s], recv.at[p, r], dev).start()

    def got(p, r, ref):
        remote(ref, ref, send.at[p, 0], recv.at[p, r], pc.partner()).wait_recv()

    def gone(p, s, ref):
        remote(ref, ref, send.at[p, s], recv.at[p, 0], pc.partner()).wait_send()

    def some(p, n):
        return ts[p].at[pl.ds(0, n * 8)]

    def meta_of(p, da):
        return mm.at[p, k[axes[p][1]], rem4(k[axes[p][0]] + da + RING)]

    def along_b(p, da):
        for dl in (1, -1):
            push(p, S_GATHER, R_SIDES + da, blk(p, da, 0), pc.peer(axes[p][1], dl))

    def b_sides(p, da):
        got(p, R_SIDES + da, some(p, 2))
        dl = 1 if da in (0, 2) else -1
        push(p, S_GATHER, R_ENDS + (da in (1, 2)), blk(p, da, 3 if dl == 1 else 1), pc.peer(axes[p][1], dl))

    def b_ends(p, n):
        got(p, R_ENDS + n, some(p, 2))

    early = rem4(k[0] + k[1] + k[2] + 2)
    row = lax.broadcasted_iota(jnp.int32, (8 * SLOTS, toks), 0)

    def pick(p, da, db):
        a, b, c = axes[p]
        aa, bb = rem4(k[a] + da), rem4(k[b] + db)
        j = rem4(aa + bb + k[c])
        first = SLOTS * (pc.me - k[c] * pc.stride[c] - pc.core)
        rows = (first + (row >> 5) * (SLOTS * pc.stride[c]) + (row & 31)).astype(F32)
        ids = mm[p, bb, aa, pl.ds(0, top_k)]
        chosen = sum(jnp.where(hit, 1.0, 0.0) for hit in slots_of(rows, ids)).astype(BF16)
        block = ts[p][pl.ds((bb * RING + aa) * 8, 8)].reshape(toks, widths[p])
        picked = jnp.dot(chosen, block, preferred_element_type=F32).astype(BF16)
        ss[p][pl.ds(j * 8, 8), bb] = picked.reshape(8, SLOTS, widths[p])

    def sides(p, da):
        @pl.loop(0, 2)
        def _(q):
            pick(p, da, 3 - 2 * q)

    to_expert = [
        Exchange(pc, axes[p][2], (lambda n, p=p: ss[p].at[n]), ls[p], send.at[p, S_C], shared, R_C) for p in range(3)
    ]
    def offer(p, j, far=True, near=True):
        line = to_expert[p]
        for cp in (line.far(j) if far else []) + (line.near(j) if near else []):
            cp.start()
        if near:
            ls[p][line.own(j)] = ss[p][line.own(j)]

    for p in range(3):
        for dl in STEPS:
            push(p, S_META, R_META, meta_of(p, 0), pc.peer(axes[p][0], dl))
        push(p, S_GATHER, R_A, blk(p, 0, 0), pc.peer(axes[p][0], 1))
        push(p, S_GATHER, R_A + 1, blk(p, 0, 0), pc.peer(axes[p][0], -1))
    for p in range(3):
        along_b(p, 0)
    for cp in weights:
        cp.start()
    with jax.named_scope("ag_meta"):
        for p in range(3):
            got(p, R_META, mm.at[p, 0, pl.ds(0, 3)])
            for dl in STEPS:
                push(p, S_META + 1, R_META + 1, mm.at[p, k[axes[p][1]], :, pl.ds(0, top_k)], pc.peer(axes[p][1], dl))
    with jax.named_scope("ag_a"):
        for p in range(3):
            got(p, R_A, blk(p, 3, 0))
            push(p, S_GATHER, R_FAR, half_blk(p, 3, 0, 0), pc.peer(axes[p][0], 1))
            got(p, R_A + 1, blk(p, 1, 0))
            push(p, S_GATHER, R_FAR, half_blk(p, 1, 0, 1), pc.peer(axes[p][0], -1))
        for p in range(3):
            along_b(p, 3)
        for p in range(3):
            along_b(p, 1)
    with jax.named_scope("pick0"):
        for p in range(3):
            @pl.loop(0, 3)
            def _(q):
                pick(p, q + lax.div(q, 2), 0)
    with jax.named_scope("ag_a2"):
        for p in range(3):
            got(p, R_FAR, blk(p, 2, 0))
            along_b(p, 2)
    with jax.named_scope("ag_b0"):
        for p in range(3):
            b_sides(p, 0)
    for p in range(3):
        got(p, R_META + 1, mm.at[p, pl.ds(0, 3), :, pl.ds(0, top_k)])
    with jax.named_scope("pick1"):
        for p in range(3):
            pick(p, 2, 0)
            sides(p, 0)
    for da in (3, 1):
        with jax.named_scope("ag_b13"):
            for p in range(3):
                b_sides(p, da)
        with jax.named_scope("pick13"):
            for p in range(3):
                sides(p, da)
    with jax.named_scope("ag_b2"):
        for p in range(3):
            b_sides(p, 2)
    with jax.named_scope("pick2"):
        for p in range(3):
            sides(p, 2)
    to_source = [
        Exchange(pc, back[p][2], (lambda n, p=p: ts[p].at[pl.ds(n * RING, RING)]), cs[p], send.at[p, S_BACK], recv.at[p], R_BACK, True)
        for p in range(3)
    ]

    for p in (2, 1, 0):
        with jax.named_scope("ag_b3"):
            b_ends(p, 0)
        with jax.named_scope("pick3"):
            @pl.loop(0, 2)
            def _(q):
                pick(p, 3 * q, 2)

            offer(p, early, near=p > 0)
    for p in (2, 1, 0):
        with jax.named_scope("ag_b4"):
            b_ends(p, 1)
        with jax.named_scope("pick4"):
            @pl.loop(0, 2)
            def _(q):
                pick(p, 1 + q, 2)

            if p:
                @pl.loop(0, RING - 1)
                def _(q):
                    offer(p, q + lax.div(q + RING - early, RING))
            else:
                @pl.loop(0, RING)
                def _(j):
                    @pl.when(j != early)
                    def _():
                        offer(p, j, near=False)

                    offer(p, j, far=False)

    def prepare(p, j, bank):
        a, b, c = back[p]
        src = rem4(j + 2 * RING - k[c] - k[b])
        first = SLOTS * (pc.me - k[b] * pc.stride[b] - k[c] * pc.stride[c] - pc.core)
        info = mm[(p + 2) % 3, k[b], src]
        rows = first + (row >> 5) * (SLOTS * pc.stride[c]) + (row & 31)

        @pl.loop(0, RING)
        def _(bb):
            hits = slots_of((rows + bb * (SLOTS * pc.stride[b])).astype(F32), info[:top_k])
            chosen = sum(jnp.where(hit, 1.0, 0.0) for hit in hits)
            gate = sum(jnp.where(hit, info[top_k + n:top_k + n + 1, :], 0.0) for n, hit in enumerate(hits))
            at = pl.ds(pl.multiple_of(bb * 8 * SLOTS, 8 * SLOTS), 8 * SLOTS)
            hot[bank, p, at] = chosen.astype(BF16)
            scale[at, 3 * bank + p:3 * bank + p + 1] = jnp.sum(gate, axis=1, keepdims=True)

    def prepared(j, bank):
        with jax.named_scope("prepare"):
            for p in range(3):
                prepare(p, j, bank)

    prepared(RING - 1, 1)
    prepared(0, 0)

    for cp in weights:
        cp.wait()
    for p in range(3):
        gone(p, S_META, mm.at[p, 0, pl.ds(0, 3)])
        gone(p, S_META + 1, mm.at[p, pl.ds(0, 3), :, pl.ds(0, top_k)])
        gone(p, S_GATHER, some(p, 15))

    def places(order, j, zy, core):
        z, yy = lax.div(zy, RING), rem4(zy)
        at = (z, yy, rem4(j + 2 * RING - z - yy))
        return [(j * 8 + at[(c + core) % 3] * 2 + core, at[(b + core) % 3]) for a, b, c in order]

    def ffn(j):
        @pl.loop(0, RING * RING)
        def _(zy):
            for core in range(2):
                for p, (at, bb) in enumerate(places(axes, j, zy, core)):
                    x[pl.ds(pl.multiple_of((zy * 2 + core) * SLOTS, SLOTS), SLOTS), pl.ds(starts[p], widths[p])] = ls[p][at, bb]

        g = jnp.dot(x[...], vg[...], preferred_element_type=F32)
        u = jnp.dot(x[...], vu[...], preferred_element_type=F32)
        hid[...] = (g * jax.nn.sigmoid(g) * u).astype(BF16)
        x[...] = jnp.dot(hid[...], vd[...], preferred_element_type=F32).astype(BF16)

        @pl.loop(0, RING * RING)
        def _(zy):
            for core in range(2):
                for p, (at, bb) in enumerate(places(back, j, zy, core)):
                    ts[p][at * RING + bb] = x[pl.ds(pl.multiple_of((zy * 2 + core) * SLOTS, SLOTS), SLOTS), pl.ds(starts[p], widths[p])]

    @pl.loop(0, RING)
    def _(j):
        with jax.named_scope("land"):
            full = x.at[pl.ds(0, 7 * RING * SLOTS)]
            remote(full, full, send.at[0, S_C], shared.at[R_C + j], pc.partner()).wait_recv()
        with jax.named_scope("ffn"):
            ffn(j)
        with jax.named_scope("send2"):
            for p, line in enumerate(to_source):
                for cp in line.sends(j):
                    cp.start()
                cs[p][line.own(j)] = ts[p][pl.ds(line.own(j) * RING, RING)]

    cut = 128 * ((widths[0] // 128 + 1) // 2)
    piece = [[pl.ds(0, cut), pl.ds(cut, w - cut)] for w in widths]

    def second(p, j):
        b = back[p][1]
        return [
            remote(cs[p].at[pl.ds(j * 8, 8), rem4(k[b] + dl + RING), :, piece[p][u]], ms[p].at[j * RING + k[b], :, :, piece[p][u]],
                   send.at[p, S_B], recv.at[p, R_B + j + u * lax.div(j, RING - 1)], pc.peer(b, dl))
            for u in range(2) for dl in STEPS
        ]

    @pl.loop(0, RING)
    def _(j):
        with jax.named_scope("land2"):
            for p, line in enumerate(to_source):
                line.wait_land(j)
                for cp in second(p, j):
                    cp.start()
        for p in range(3):
            kb = k[back[p][1]]
            ms[p][j * RING + kb] = cs[p][pl.ds(j * 8, 8), kb]

    def combine(p, j, cols, bank):
        a, b, c = back[p]
        src = rem4(j + 2 * RING - k[c] - k[b])
        xcols = pl.ds(starts[p] + cols.start, cols.size)

        @pl.loop(0, RING)
        def _(bb):
            at = pl.ds(pl.multiple_of(bb * 8 * SLOTS, 8 * SLOTS), 8 * SLOTS)
            rows = ms[p][j * RING + bb, :, :, cols].reshape(8 * SLOTS, cols.size)
            x[at, xcols] = (rows.astype(F32) * scale[at, 3 * bank + p:3 * bank + p + 1]).astype(BF16)

        sums[p][src, :, cols] = lax.dot_general(hot[bank, p], x[:, xcols], (((0,), (0,)), ((), ())), preferred_element_type=F32)

    @pl.loop(0, RING - 1)
    def _(j):
        for p in range(3):
            with jax.named_scope("arrive"):
                got(p, R_B + j, ms[p].at[pl.ds(j * RING, 3)])
            with jax.named_scope("combine"):
                combine(p, j, pl.ds(0, widths[p]), 0)

        @pl.when(j < RING - 2)
        def _():
            prepared(j + 1, 0)


    def hand(p, r, ref, dst, dl):
        remote(ref, dst, send.at[p, S_SUM], recv.at[p, R_SUM + r], pc.peer(back[p][0], dl)).start()

    sides_of = ((0, 1), (1, -1))
    for u in range(2):
        for p in range(3):
            cols = piece[p][u]
            with jax.named_scope("arrive"):
                got(p, R_B + RING - 1 + u, ms[p].at[pl.ds((RING - 1) * RING, 3), :, :, cols])
            with jax.named_scope("combine"):
                combine(p, RING - 1, cols, 1)
            ka = k[back[p][0]]
            for d, dl in sides_of:
                hand(p, u, sums[p].at[rem4(ka + 2), pl.ds(d * half, half), cols], fars[p].at[d, :, cols], dl)
            for d, dl in sides_of:
                rows = pl.ds((1 - d) * half, half)
                hand(p, 2 + u, sums[p].at[rem4(ka + dl + RING), rows, cols], nears[p].at[d, rows, cols], dl)
    for u in range(2):
        with jax.named_scope("rs1"):
            for p in range(3):
                cols = piece[p][u]
                ka = k[back[p][0]]
                got(p, R_SUM + u, fars[p].at[:, :, cols])
                for d, dl in sides_of:
                    near = rem4(ka + dl + RING)
                    rows = pl.ds(d * half, half)
                    sums[p][near, rows, cols] = sums[p][near, rows, cols] + fars[p][d, :, cols]
                    hand(p, 2 + u, sums[p].at[near, rows, cols], nears[p].at[d, rows, cols], dl)
    for u in range(2):
        with jax.named_scope("rs2"):
            for p in range(3):
                cols = piece[p][u]
                got(p, R_SUM + 2 + u, nears[p].at[:, :, cols])
                total = sums[p][k[back[p][0]], :, cols] + nears[p][0, :, cols] + nears[p][1, :, cols]
                out[:, pl.ds(starts[p] + cols.start, cols.size)] = total.astype(out.dtype)
    with jax.named_scope("drain"):
        for p in range(3):
            to_expert[p].wait_sent()
            to_source[p].wait_sent()
            gone(p, S_B, ms[p].at[pl.ds(0, 3 * RING)])
            gone(p, S_SUM, sums[p].at[pl.ds(0, 3)])


def solution(mesh):
    row_spec = P(("data", "expert"), None)
    weight_spec = P("expert", None, None)
    any_spec = pl.BlockSpec(memory_space=pl.ANY)

    def device_layer(tokens, expert_ids, gate_wts, dev_slot, exp_slot, w_gate, w_up, w_down):
        toks, top_k = expert_ids.shape
        d_model, d_ff = w_gate.shape[1:]
        tiles = d_model // 128
        widths = [128 * (tiles - 2 * (tiles // 3)), 128 * (tiles // 3), 128 * (tiles // 3)]
        starts = [0, widths[0], widths[0] + widths[1]]
        dims = (widths, starts)
        n_blocks = 2 * RING * RING

        def bufs(*lead, dtype=BF16):
            return [pltpu.VMEM((*lead, w), dtype) for w in widths]

        summed = pl.pallas_call(
            lambda *refs: layer_kernel(dims, *refs),
            out_shape=pltpu.VMEM((toks, d_model), BF16),
            in_specs=[any_spec] * 8,
            out_specs=pl.BlockSpec(memory_space=pltpu.VMEM),
            scratch_shapes=[
                *bufs(n_blocks * RING, SLOTS),
                pltpu.VMEM((3, RING, RING, 2 * top_k, toks), F32),
                *bufs(n_blocks, RING, SLOTS),
                *bufs(n_blocks, RING, SLOTS),
                pltpu.VMEM((n_blocks * SLOTS, d_model), BF16),
                pltpu.VMEM((n_blocks * SLOTS, d_ff), BF16),
                pltpu.VMEM((d_model, d_ff), BF16),
                pltpu.VMEM((d_model, d_ff), BF16),
                pltpu.VMEM((d_ff, d_model), BF16),
                *bufs(n_blocks, RING, SLOTS),
                *bufs(RING * RING, 8, SLOTS),
                *bufs(RING, toks, dtype=F32),
                *bufs(2, toks // 2, dtype=F32),
                *bufs(2, toks, dtype=F32),
                pltpu.VMEM((2, 3, n_blocks * SLOTS, toks), BF16),
                pltpu.VMEM((n_blocks * SLOTS, 6), F32),
                pltpu.VMEM((3, top_k, toks), jnp.int32),
                pltpu.VMEM((top_k, toks), F32),
                pltpu.SemaphoreType.DMA((3, N_SEND)),
                pltpu.SemaphoreType.DMA((3, N_RECV)),
                pltpu.SemaphoreType.DMA((RING,)),
                pltpu.SemaphoreType.DMA((10,)),
            ],
            compiler_params=pltpu.CompilerParams(collective_id=0, has_side_effects=True, vmem_limit_bytes=VMEM_CAP),
            name="moe_layer",
        )(tokens.reshape(toks // SLOTS, SLOTS, d_model), expert_ids.T, dev_slot.T, exp_slot.T, gate_wts.T, w_gate, w_up, w_down)
        return summed

    def moe_layer(*args):
        return jax.shard_map(device_layer, mesh=mesh, in_specs=(row_spec,) * 5 + (weight_spec,) * 3, out_specs=row_spec, check_vma=False)(*args)

    return moe_layer
```

```python
import jax
import jax.numpy as jnp
from jax import lax
from jax.experimental import pallas as pl
from jax.experimental.pallas import tpu as pltpu
from jax.sharding import PartitionSpec as P

STRIDE = (32, 8, 2)
RING = 4
SLOTS = 16
STEPS = (2, 1, -1)
VMEM_CAP = 66400000
BF16 = jnp.bfloat16
F32 = jnp.float32


def rem4(v):
    return lax.rem(v, RING)


class Place:
    def __init__(self):
        self.me = lax.axis_index("expert")
        self.core = lax.rem(self.me, 2)
        self.grid = [rem4(lax.div(self.me, s)) for s in STRIDE]
        self.k, self.stride = self.turned(self.grid), self.turned(STRIDE)

    def turned(self, of):
        return [of[i] + self.core * (of[(i + 1) % 3] - of[i]) for i in range(3)]

    def peer(self, axis, delta, core=None):
        there = rem4(self.k[axis] + delta + RING)
        dev = self.me + (there - self.k[axis]) * self.stride[axis]
        return dev if core is None else dev + core - self.core

    def partner(self):
        return self.me + 1 - 2 * self.core

    def greet(self):
        sem = pltpu.get_barrier_semaphore()
        peers = [self.peer(ax, dl, c) for ax in range(3) for dl in STEPS for c in (0, 1)] + [self.partner()]
        self.n_peers = len(peers)
        for dev in peers:
            pl.semaphore_signal(sem, inc=1, device_id={"expert": dev}, device_id_type=pl.DeviceIdType.MESH)

    def meet(self):
        pl.semaphore_wait(pltpu.get_barrier_semaphore(), self.n_peers)


def remote(src, dst, send, recv, dev):
    return pltpu.make_async_remote_copy(
        src_ref=src, dst_ref=dst, send_sem=send, recv_sem=recv, device_id={"expert": dev}, device_id_type=pl.DeviceIdType.MESH
    )


class Exchange:
    def __init__(self, pc, c, block, land, send, recv, base, by_target=False):
        self.pc, self.c, self.block, self.land = pc, c, block, land
        self.send, self.recv, self.base = send, recv, base
        ours = pc.k[c], pc.stride[c]
        if by_target:
            turn = [(c + core) % 3 for core in range(2)]
            self.ring = [(pc.grid[ax], STRIDE[ax]) for ax in turn]
            self.beside = pc.grid[turn[1]] + pc.core * (pc.grid[turn[0]] - pc.grid[turn[1]])
        else:
            self.ring = [ours, ours]
            self.beside = pc.k[c]

    def slot(self, j, at):
        return j * 8 + at * 2 + self.pc.core

    def own(self, j):
        return self.slot(j, self.pc.k[self.c])

    def far(self, j):
        return self.to_ring(j, 2)

    def near(self, j):
        pc = self.pc
        sems = self.send, self.recv.at[self.base + j]
        across = remote(self.block(j * 8 + self.beside * 2 + 1 - pc.core), self.land.at[self.slot(j, self.beside)], *sems, pc.partner())
        return self.to_ring(j, 1) + self.to_ring(j, -1) + [across]

    def to_ring(self, j, dl):
        pc = self.pc
        sems = self.send, self.recv.at[self.base + j]
        out = []
        for core, (at, stride) in enumerate(self.ring):
            there = rem4(at + dl + RING)
            dev = pc.me + (there - at) * stride + core - pc.core
            out.append(remote(self.block(j * 8 + there * 2 + core), self.land.at[self.slot(j, at)], *sems, dev))
        return out

    def sends(self, j):
        return self.far(j) + self.near(j)

    def wait_land(self, j):
        rows = self.land.at[pl.ds(j * 8, 7)]
        remote(rows, rows, self.send, self.recv.at[self.base + j], self.pc.partner()).wait_recv()

    def wait_sent(self):
        rows = self.land.at[pl.ds(0, 7 * RING)]
        remote(rows, rows, self.send, self.recv.at[self.base], self.pc.partner()).wait_send()


def slots_of(rows, ids):
    return [ids[n:n + 1, :] == rows for n in range(ids.shape[0])]


R_META, R_A, R_FAR, R_SIDES, R_ENDS, R_BACK, R_B, R_SUM, N_RECV = 0, 2, 4, 5, 9, 11, 15, 20, 24
R_C = 0
S_META, S_GATHER, S_C, S_BACK, S_B, S_SUM, N_SEND = 0, 2, 3, 4, 5, 6, 7


def layer_kernel(dims, tok, ids, devs, exps, gates, wg, wu, wd, out, t0, t1, t2, mm, s0, s1, s2, l0, l1, l2, x, hid, vg, vu, vd, c0, c1, c2,
                 m0, m1, m2, a0, a1, a2, f0, f1, f2, g0, g1, g2, hot, scale, raw, hot_gate, send, recv, shared, here):
    widths, starts = dims
    pc = Place()
    ts, ss, ls, cs, ms, sums = (t0, t1, t2), (s0, s1, s2), (l0, l1, l2), (c0, c1, c2), (m0, m1, m2), (a0, a1, a2)
    fars, nears = (f0, f1, f2), (g0, g1, g2)
    axes = [(p, (p + 1) % 3, (p + 2) % 3) for p in range(3)]
    back = [axes[(p + 2) % 3] for p in range(3)]
    k = pc.k
    toks = mm.shape[-1]
    top_k = ids.shape[0]
    half = toks // 2

    def spot(p, da, db):
        a, b, c = axes[p]
        return rem4(k[b] + db) * RING + rem4(k[a] + da)

    def blk(p, da, db):
        return ts[p].at[pl.ds(spot(p, da, db) * 8, 8)]

    def half_blk(p, da, db, d):
        return ts[p].at[pl.ds(spot(p, da, db) * 8 + d * 4, 4)]

    loads = [
        pltpu.make_async_copy(tok.at[:, :, pl.ds(starts[p], widths[p])], blk(p, 0, 0), here.at[0]) for p in range(3)
    ]
    routes = [pltpu.make_async_copy(src, raw.at[n], here.at[4]) for n, src in enumerate((ids, devs, exps))]
    routes.append(pltpu.make_async_copy(gates, hot_gate, here.at[4]))
    weights = [pltpu.make_async_copy(src.at[0], dst, here.at[1 + n]) for n, (src, dst) in enumerate(((wg, vg), (wu, vu), (wd, vd)))]
    for cp in routes + loads:
        cp.start()
    with jax.named_scope("barrier"):
        pc.greet()
        four = mm.at[0, 0, pl.ds(0, 2)]
        pltpu.make_async_copy(four, four, here.at[4]).wait()
        kept = (raw[1] >= 0) & (raw[2] >= 0)
        dest = jnp.where(kept, raw[0] * SLOTS + raw[1], -1).astype(F32)
        gate_bf = hot_gate[...].astype(BF16).astype(F32)
        for p, (a, b, c) in enumerate(axes):
            mm[p, k[b], k[a], pl.ds(0, top_k)] = dest
            mm[p, k[b], k[a], pl.ds(top_k, top_k)] = gate_bf
        mine = x.at[pl.ds(0, toks)]
        pltpu.make_async_copy(mine, mine, here.at[0]).wait()
        pc.meet()

    def push(p, s, r, ref, dev):
        remote(ref, ref, send.at[p, s], recv.at[p, r], dev).start()

    def got(p, r, ref):
        remote(ref, ref, send.at[p, 0], recv.at[p, r], pc.partner()).wait_recv()

    def gone(p, s, ref):
        remote(ref, ref, send.at[p, s], recv.at[p, 0], pc.partner()).wait_send()

    def some(p, n):
        return ts[p].at[pl.ds(0, n * 8)]

    def meta_of(p, da):
        return mm.at[p, k[axes[p][1]], rem4(k[axes[p][0]] + da + RING)]

    def along_b(p, da):
        for dl in (1, -1):
            push(p, S_GATHER, R_SIDES + da, blk(p, da, 0), pc.peer(axes[p][1], dl))

    def b_sides(p, da):
        got(p, R_SIDES + da, some(p, 2))
        dl = 1 if da in (0, 2) else -1
        push(p, S_GATHER, R_ENDS + (da in (1, 2)), blk(p, da, 3 if dl == 1 else 1), pc.peer(axes[p][1], dl))

    def b_ends(p, n):
        got(p, R_ENDS + n, some(p, 2))

    early = rem4(k[0] + k[1] + k[2] + 2)
    row = lax.broadcasted_iota(jnp.int32, (8 * SLOTS, toks), 0)

    def pick(p, da, db):
        a, b, c = axes[p]
        aa, bb = rem4(k[a] + da), rem4(k[b] + db)
        j = rem4(aa + bb + k[c])
        first = SLOTS * (pc.me - k[c] * pc.stride[c] - pc.core)
        rows = (first + (row >> 5) * (SLOTS * pc.stride[c]) + (row & 31)).astype(F32)
        ids = mm[p, bb, aa, pl.ds(0, top_k)]
        chosen = sum(jnp.where(hit, 1.0, 0.0) for hit in slots_of(rows, ids)).astype(BF16)
        block = ts[p][pl.ds((bb * RING + aa) * 8, 8)].reshape(toks, widths[p])
        picked = jnp.dot(chosen, block, preferred_element_type=F32).astype(BF16)
        ss[p][pl.ds(j * 8, 8), bb] = picked.reshape(8, SLOTS, widths[p])

    def sides(p, da):
        @pl.loop(0, 2)
        def _(q):
            pick(p, da, 3 - 2 * q)

    to_expert = [
        Exchange(pc, axes[p][2], (lambda n, p=p: ss[p].at[n]), ls[p], send.at[p, S_C], shared, R_C) for p in range(3)
    ]
    def offer(p, j, far=True, near=True):
        line = to_expert[p]
        for cp in (line.far(j) if far else []) + (line.near(j) if near else []):
            cp.start()
        if near:
            ls[p][line.own(j)] = ss[p][line.own(j)]

    for p in range(3):
        for dl in STEPS:
            push(p, S_META, R_META, meta_of(p, 0), pc.peer(axes[p][0], dl))
        push(p, S_GATHER, R_A, blk(p, 0, 0), pc.peer(axes[p][0], 1))
        push(p, S_GATHER, R_A + 1, blk(p, 0, 0), pc.peer(axes[p][0], -1))
    for p in range(3):
        along_b(p, 0)
    for cp in weights:
        cp.start()
    with jax.named_scope("ag_meta"):
        for p in range(3):
            got(p, R_META, mm.at[p, 0, pl.ds(0, 3)])
            for dl in STEPS:
                push(p, S_META + 1, R_META + 1, mm.at[p, k[axes[p][1]], :, pl.ds(0, top_k)], pc.peer(axes[p][1], dl))
    with jax.named_scope("ag_a"):
        for p in range(3):
            got(p, R_A, blk(p, 3, 0))
            push(p, S_GATHER, R_FAR, half_blk(p, 3, 0, 0), pc.peer(axes[p][0], 1))
            got(p, R_A + 1, blk(p, 1, 0))
            push(p, S_GATHER, R_FAR, half_blk(p, 1, 0, 1), pc.peer(axes[p][0], -1))
        for p in range(3):
            along_b(p, 3)
        for p in range(3):
            along_b(p, 1)
    with jax.named_scope("pick0"):
        for p in range(3):
            @pl.loop(0, 3)
            def _(q):
                pick(p, q + lax.div(q, 2), 0)
    with jax.named_scope("ag_a2"):
        for p in range(3):
            got(p, R_FAR, blk(p, 2, 0))
            along_b(p, 2)
    with jax.named_scope("ag_b0"):
        for p in range(3):
            b_sides(p, 0)
    for p in range(3):
        got(p, R_META + 1, mm.at[p, pl.ds(0, 3), :, pl.ds(0, top_k)])
    with jax.named_scope("pick1"):
        for p in range(3):
            pick(p, 2, 0)
            sides(p, 0)
    for da in (3, 1):
        with jax.named_scope("ag_b13"):
            for p in range(3):
                b_sides(p, da)
        with jax.named_scope("pick13"):
            for p in range(3):
                sides(p, da)
    with jax.named_scope("ag_b2"):
        for p in range(3):
            b_sides(p, 2)
    with jax.named_scope("pick2"):
        for p in range(3):
            sides(p, 2)
    to_source = [
        Exchange(pc, back[p][2], (lambda n, p=p: ts[p].at[pl.ds(n * RING, RING)]), cs[p], send.at[p, S_BACK], recv.at[p], R_BACK, True)
        for p in range(3)
    ]

    for p in (2, 1, 0):
        with jax.named_scope("ag_b3"):
            b_ends(p, 0)
        with jax.named_scope("pick3"):
            @pl.loop(0, 2)
            def _(q):
                pick(p, 3 * q, 2)

            offer(p, early, near=p > 0)
    for p in (2, 1, 0):
        with jax.named_scope("ag_b4"):
            b_ends(p, 1)
        with jax.named_scope("pick4"):
            @pl.loop(0, 2)
            def _(q):
                pick(p, 1 + q, 2)

            if p:
                @pl.loop(0, RING - 1)
                def _(q):
                    offer(p, q + lax.div(q + RING - early, RING))
            else:
                @pl.loop(0, RING)
                def _(j):
                    @pl.when(j != early)
                    def _():
                        offer(p, j, near=False)

                    offer(p, j, far=False)

    def prepare(p, j, bank):
        a, b, c = back[p]
        src = rem4(j + 2 * RING - k[c] - k[b])
        first = SLOTS * (pc.me - k[b] * pc.stride[b] - k[c] * pc.stride[c] - pc.core)
        info = mm[(p + 2) % 3, k[b], src]
        rows = first + (row >> 5) * (SLOTS * pc.stride[c]) + (row & 31)

        @pl.loop(0, RING)
        def _(bb):
            hits = slots_of((rows + bb * (SLOTS * pc.stride[b])).astype(F32), info[:top_k])
            chosen = sum(jnp.where(hit, 1.0, 0.0) for hit in hits)
            gate = sum(jnp.where(hit, info[top_k + n:top_k + n + 1, :], 0.0) for n, hit in enumerate(hits))
            at = pl.ds(pl.multiple_of(bb * 8 * SLOTS, 8 * SLOTS), 8 * SLOTS)
            hot[bank, p, at] = chosen.astype(BF16)
            scale[at, 3 * bank + p:3 * bank + p + 1] = jnp.sum(gate, axis=1, keepdims=True)

    def prepared(j, bank):
        with jax.named_scope("prepare"):
            for p in range(3):
                prepare(p, j, bank)

    prepared(RING - 1, 1)
    prepared(0, 0)

    for cp in weights:
        cp.wait()
    for p in range(3):
        gone(p, S_META, mm.at[p, 0, pl.ds(0, 3)])
        gone(p, S_META + 1, mm.at[p, pl.ds(0, 3), :, pl.ds(0, top_k)])
        gone(p, S_GATHER, some(p, 15))

    def places(order, j, zy, core):
        z, yy = lax.div(zy, RING), rem4(zy)
        at = (z, yy, rem4(j + 2 * RING - z - yy))
        return [(j * 8 + at[(c + core) % 3] * 2 + core, at[(b + core) % 3]) for a, b, c in order]

    def ffn(j):
        @pl.loop(0, RING * RING)
        def _(zy):
            for core in range(2):
                for p, (at, bb) in enumerate(places(axes, j, zy, core)):
                    x[pl.ds(pl.multiple_of((zy * 2 + core) * SLOTS, SLOTS), SLOTS), pl.ds(starts[p], widths[p])] = ls[p][at, bb]

        g = jnp.dot(x[...], vg[...], preferred_element_type=F32)
        u = jnp.dot(x[...], vu[...], preferred_element_type=F32)
        hid[...] = (g * jax.nn.sigmoid(g) * u).astype(BF16)
        x[...] = jnp.dot(hid[...], vd[...], preferred_element_type=F32).astype(BF16)

        @pl.loop(0, RING * RING)
        def _(zy):
            for core in range(2):
                for p, (at, bb) in enumerate(places(back, j, zy, core)):
                    ts[p][at * RING + bb] = x[pl.ds(pl.multiple_of((zy * 2 + core) * SLOTS, SLOTS), SLOTS), pl.ds(starts[p], widths[p])]

    @pl.loop(0, RING)
    def _(j):
        with jax.named_scope("land"):
            full = x.at[pl.ds(0, 7 * RING * SLOTS)]
            remote(full, full, send.at[0, S_C], shared.at[R_C + j], pc.partner()).wait_recv()
        with jax.named_scope("ffn"):
            ffn(j)
        with jax.named_scope("send2"):
            for p, line in enumerate(to_source):
                for cp in line.sends(j):
                    cp.start()
                cs[p][line.own(j)] = ts[p][pl.ds(line.own(j) * RING, RING)]

    cut = 128 * ((widths[0] // 128 + 1) // 2)
    piece = [[pl.ds(0, cut), pl.ds(cut, w - cut)] for w in widths]

    def second(p, j):
        b = back[p][1]
        return [
            remote(cs[p].at[pl.ds(j * 8, 8), rem4(k[b] + dl + RING), :, piece[p][u]], ms[p].at[j * RING + k[b], :, :, piece[p][u]],
                   send.at[p, S_B], recv.at[p, R_B + j + u * lax.div(j, RING - 1)], pc.peer(b, dl))
            for u in range(2) for dl in STEPS
        ]

    @pl.loop(0, RING)
    def _(j):
        with jax.named_scope("land2"):
            for p, line in enumerate(to_source):
                line.wait_land(j)
                for cp in second(p, j):
                    cp.start()
        for p in range(3):
            kb = k[back[p][1]]
            ms[p][j * RING + kb] = cs[p][pl.ds(j * 8, 8), kb]

    def combine(p, j, cols, bank):
        a, b, c = back[p]
        src = rem4(j + 2 * RING - k[c] - k[b])
        xcols = pl.ds(starts[p] + cols.start, cols.size)

        @pl.loop(0, RING)
        def _(bb):
            at = pl.ds(pl.multiple_of(bb * 8 * SLOTS, 8 * SLOTS), 8 * SLOTS)
            rows = ms[p][j * RING + bb, :, :, cols].reshape(8 * SLOTS, cols.size)
            x[at, xcols] = (rows.astype(F32) * scale[at, 3 * bank + p:3 * bank + p + 1]).astype(BF16)

        sums[p][src, :, cols] = lax.dot_general(hot[bank, p], x[:, xcols], (((0,), (0,)), ((), ())), preferred_element_type=F32)

    @pl.loop(0, RING - 1)
    def _(j):
        for p in range(3):
            with jax.named_scope("arrive"):
                got(p, R_B + j, ms[p].at[pl.ds(j * RING, 3)])
            with jax.named_scope("combine"):
                combine(p, j, pl.ds(0, widths[p]), 0)

        @pl.when(j < RING - 2)
        def _():
            prepared(j + 1, 0)


    def hand(p, r, ref, dst, dl):
        remote(ref, dst, send.at[p, S_SUM], recv.at[p, R_SUM + r], pc.peer(back[p][0], dl)).start()

    sides_of = ((0, 1), (1, -1))
    for u in range(2):
        for p in range(3):
            cols = piece[p][u]
            with jax.named_scope("arrive"):
                got(p, R_B + RING - 1 + u, ms[p].at[pl.ds((RING - 1) * RING, 3), :, :, cols])
            with jax.named_scope("combine"):
                combine(p, RING - 1, cols, 1)
            ka = k[back[p][0]]
            for d, dl in sides_of:
                hand(p, u, sums[p].at[rem4(ka + 2), pl.ds(d * half, half), cols], fars[p].at[d, :, cols], dl)
            for d, dl in sides_of:
                rows = pl.ds((1 - d) * half, half)
                hand(p, 2 + u, sums[p].at[rem4(ka + dl + RING), rows, cols], nears[p].at[d, rows, cols], dl)
    for u in range(2):
        with jax.named_scope("rs1"):
            for p in range(3):
                cols = piece[p][u]
                ka = k[back[p][0]]
                got(p, R_SUM + u, fars[p].at[:, :, cols])
                for d, dl in sides_of:
                    near = rem4(ka + dl + RING)
                    rows = pl.ds(d * half, half)
                    sums[p][near, rows, cols] = sums[p][near, rows, cols] + fars[p][d, :, cols]
                    hand(p, 2 + u, sums[p].at[near, rows, cols], nears[p].at[d, rows, cols], dl)
    for u in range(2):
        with jax.named_scope("rs2"):
            for p in range(3):
                cols = piece[p][u]
                got(p, R_SUM + 2 + u, nears[p].at[:, :, cols])
                total = sums[p][k[back[p][0]], :, cols] + nears[p][0, :, cols] + nears[p][1, :, cols]
                out[:, pl.ds(starts[p] + cols.start, cols.size)] = total.astype(out.dtype)
    with jax.named_scope("drain"):
        for p in range(3):
            to_expert[p].wait_sent()
            to_source[p].wait_sent()
            gone(p, S_B, ms[p].at[pl.ds(0, 3 * RING)])
            gone(p, S_SUM, sums[p].at[pl.ds(0, 3)])


def solution(mesh):
    row_spec = P(("data", "expert"), None)
    weight_spec = P("expert", None, None)
    any_spec = pl.BlockSpec(memory_space=pl.ANY)

    def device_layer(tokens, expert_ids, gate_wts, dev_slot, exp_slot, w_gate, w_up, w_down):
        toks, top_k = expert_ids.shape
        d_model, d_ff = w_gate.shape[1:]
        tiles = d_model // 128
        widths = [128 * (tiles - 2 * (tiles // 3)), 128 * (tiles // 3), 128 * (tiles // 3)]
        starts = [0, widths[0], widths[0] + widths[1]]
        dims = (widths, starts)
        n_blocks = 2 * RING * RING

        def bufs(*lead, dtype=BF16):
            return [pltpu.VMEM((*lead, w), dtype) for w in widths]

        summed = pl.pallas_call(
            lambda *refs: layer_kernel(dims, *refs),
            out_shape=pltpu.VMEM((toks, d_model), BF16),
            in_specs=[any_spec] * 8,
            out_specs=pl.BlockSpec(memory_space=pltpu.VMEM),
            scratch_shapes=[
                *bufs(n_blocks * RING, SLOTS),
                pltpu.VMEM((3, RING, RING, 2 * top_k, toks), F32),
                *bufs(n_blocks, RING, SLOTS),
                *bufs(n_blocks, RING, SLOTS),
                pltpu.VMEM((n_blocks * SLOTS, d_model), BF16),
                pltpu.VMEM((n_blocks * SLOTS, d_ff), BF16),
                pltpu.VMEM((d_model, d_ff), BF16),
                pltpu.VMEM((d_model, d_ff), BF16),
                pltpu.VMEM((d_ff, d_model), BF16),
                *bufs(n_blocks, RING, SLOTS),
                *bufs(RING * RING, 8, SLOTS),
                *bufs(RING, toks, dtype=F32),
                *bufs(2, toks // 2, dtype=F32),
                *bufs(2, toks, dtype=F32),
                pltpu.VMEM((2, 3, n_blocks * SLOTS, toks), BF16),
                pltpu.VMEM((n_blocks * SLOTS, 6), F32),
                pltpu.VMEM((3, top_k, toks), jnp.int32),
                pltpu.VMEM((top_k, toks), F32),
                pltpu.SemaphoreType.DMA((3, N_SEND)),
                pltpu.SemaphoreType.DMA((3, N_RECV)),
                pltpu.SemaphoreType.DMA((RING,)),
                pltpu.SemaphoreType.DMA((5,)),
            ],
            compiler_params=pltpu.CompilerParams(collective_id=0, has_side_effects=True, vmem_limit_bytes=VMEM_CAP),
            name="moe_layer",
        )(tokens.reshape(toks // SLOTS, SLOTS, d_model), expert_ids.T, dev_slot.T, exp_slot.T, gate_wts.T, w_gate, w_up, w_down)
        return summed

    def moe_layer(*args):
        return jax.shard_map(device_layer, mesh=mesh, in_specs=(row_spec,) * 5 + (weight_spec,) * 3, out_specs=row_spec, check_vma=False)(*args)

    return moe_layer
```
